32 devices in a mesh: ctx: 8 (over y, x, core), tp: 4 (over z).
Axes of the slice: x: 2, y: 2, z: 4, core: 2. Of those that a mesh axis runs over, the one named last changes fastest.
Arguments:
- span_rows: bfloat16 [2, 256, 3584], P(None, 'ctx'), may hold values from -6 to 6
- step_rows: bfloat16 [4, 32, 3584], P(None, 'ctx'), may hold values from -6 to 6
- lengths: int32 [2], replicated, may hold values from 513 to 768
- sample_prompt: int32 [32], P('ctx'), may hold values from 0 to 1
- norm_gain: float32 [3584], replicated, may hold values from 0.5 to 1.5
- query_weight: bfloat16 [3584, 3584], P('ctx', 'tp'), may hold values from -0.1875 to 0.1875
- key_weight: bfloat16 [3584, 512], P(None, 'tp'), may hold values from -0.1875 to 0.1875
- value_weight: bfloat16 [3584, 512], P(None, 'tp'), may hold values from -0.09375 to 0.09375
- query_bias: float32 [3584], P('tp'), may hold values from -16 to 16
- key_bias: float32 [512], P('tp'), may hold values from -16 to 16
- value_bias: float32 [512], P('tp'), may hold values from -3 to 3
- out_weight: bfloat16 [3584, 3584], P('tp', 'ctx'), may hold values from -0.25 to 0.25
- cache_keys: bfloat16 [2, 512, 512], P(None, 'ctx', 'tp'), may hold values from -12 to 12
- cache_values: bfloat16 [2, 512, 512], P(None, 'ctx', 'tp'), may hold values from -6 to 6
Outputs:
- span_out: bfloat16 [2, 256, 3584], P(None, 'ctx', 'tp')
- dec_out: bfloat16 [4, 32, 3584], P(None, 'ctx', 'tp')
The draws below stay inside these ranges and needn't reach their ends.
All inputs are finite; a program needn't handle non-finite values.
Results may differ from the reference program's by a relative error of at most 0.012.
The reference program's roundings to bfloat16 on the way count: a program that leaves them out, or rounds other values in their place, can miss the bound.
Values may be sent and summed in bfloat16 or wider, within the bound.
No kernel may reach another device: no remote copies, remote signals or barrier semaphores. Data moves between devices by JAX's collectives and lax.ppermute only.
A program may use at most 128 MiB of HBM per device.

```python
import math
import jax
import jax.numpy as jnp
from jax import lax

D = 3584
HEADS = 28
KV_HEADS = 4
HEAD = 128
PROMPTS = 2
STEPS = 4
PREFIX = 512
SPAN = 256
SAMPLES = 32


def lifted_bias(key, count):
    base = jnp.clip(0.5 * jax.random.normal(key, (count, HEAD), jnp.float32), -3.0, 3.0)
    return base.reshape(count * HEAD)


def draw_query_bias(key, part):
    return lifted_bias(jax.random.fold_in(key, 11), HEADS)


def draw_key_bias(key, part):
    return lifted_bias(jax.random.fold_in(key, 23), KV_HEADS)


def with_ends(drawn, own_key, low, high):
    spot = [jax.random.randint(jax.random.fold_in(own_key, axis), (), 0, length) for axis, length in enumerate(drawn.shape)]
    widest = drawn.shape.index(max(drawn.shape))
    beside = spot[:widest] + [(spot[widest] + 1) % drawn.shape[widest]] + spot[widest + 1:]
    return drawn.at[tuple(spot)].set(low).at[tuple(beside)].set(high)


def steps_of(stream_key, dims, cuts, low, top_value):
    loudness = 1.0
    for axis_at, shards_of in cuts:
        heights = jax.random.uniform(jax.random.fold_in(jax.random.fold_in(stream_key, 6), axis_at), (shards_of,), jnp.float32, low / len(cuts), top_value / len(cuts))
        loudness = loudness * jnp.repeat(jnp.exp(heights), dims[axis_at] // shards_of).reshape((-1,) + (1,) * (len(dims) - 1 - axis_at))
    return loudness


def scatter_about(rng, dims, deviation, limit, shards=(), kind=jnp.bfloat16):
    loudness = steps_of(rng, dims, shards, -0.22, 0.18) if shards else 1.0
    entries = jax.random.normal(rng, dims, jnp.float32) * deviation * loudness
    return jnp.minimum(jnp.maximum(entries, -limit), limit).astype(kind)


def setup_inputs(seed: int = 0) -> dict:
    seeds = jax.random.split(jax.random.key(seed), 15)
    span_rows = scatter_about(seeds[0], (PROMPTS, SPAN, D), 1.0, 6.0, ((1, 8),))
    step_rows = scatter_about(seeds[1], (STEPS, SAMPLES, D), 1.0, 6.0, ((1, 8),))
    lengths = jax.random.randint(seeds[2], (PROMPTS,), PREFIX + 1, PREFIX + SPAN + 1).astype(jnp.int32)
    sample_prompt = with_ends(jax.random.randint(seeds[3], (SAMPLES,), 0, PROMPTS), jax.random.fold_in(seeds[3], 1), 0, PROMPTS - 1).astype(jnp.int32)
    norm_gain = jnp.clip(1.0 + 0.1 * jax.random.normal(seeds[4], (D,), jnp.float32), 0.5, 1.5)
    query_weight = scatter_about(seeds[5], (D, HEADS * HEAD), (D // 4) ** -0.5, 0.1875, ((0, 8), (1, 4)))
    key_weight = scatter_about(seeds[6], (D, KV_HEADS * HEAD), (D // 4) ** -0.5, 0.1875, ((1, 4),))
    value_weight = scatter_about(seeds[7], (D, KV_HEADS * HEAD), D ** -0.5, 0.09375, ((1, 4),))
    query_bias = draw_query_bias(jax.random.fold_in(seeds[14], 71), 0)
    key_bias = draw_key_bias(jax.random.fold_in(seeds[14], 71), 0)
    value_bias = scatter_about(seeds[10], (KV_HEADS * HEAD,), 0.5, 3.0, ((0, 4),), jnp.float32)
    out_weight = scatter_about(seeds[11], (HEADS * HEAD, D), (HEADS * HEAD // 8) ** -0.5, 0.25, ((0, 4), (1, 8)))
    cache_keys = scatter_about(seeds[12], (PROMPTS, PREFIX, KV_HEADS * HEAD), 2.0, 12.0, ((1, 8), (2, 4)))
    cache_values = scatter_about(seeds[13], (PROMPTS, PREFIX, KV_HEADS * HEAD), 1.0, 6.0, ((1, 8), (2, 4)))
    return {"span_rows": span_rows, "step_rows": step_rows, "lengths": lengths, "sample_prompt": sample_prompt, "norm_gain": norm_gain, "query_weight": query_weight, "key_weight": key_weight, "value_weight": value_weight, "query_bias": query_bias, "key_bias": key_bias, "value_bias": value_bias, "out_weight": out_weight, "cache_keys": cache_keys, "cache_values": cache_values}


ROPE_BASE = 1000000.0
NORM_EPS = 1e-06
MASKED = -1e+30

def norm_rows(inputs, norm_gain):
    widened = inputs.astype(jnp.float32)
    inverse = lax.rsqrt(lax.optimization_barrier(jnp.mean(widened * widened, axis=-1, keepdims=True)) + NORM_EPS)
    return (widened * inverse * norm_gain).astype(jnp.bfloat16)

def rotate(vectors, positions):
    width = vectors.shape[-1]
    half = width // 2
    exponent = jnp.arange(half, dtype=jnp.float32) * (2.0 / width)
    frequency = jnp.exp(exponent * -math.log(ROPE_BASE))
    angles = positions.astype(jnp.float32)[..., None, None] * frequency
    cosine = jnp.cos(angles)
    sine = jnp.sin(angles)
    first = vectors[..., :half]
    second = vectors[..., half:]
    return jnp.concatenate([first * cosine - second * sine, second * cosine + first * sine], axis=-1)

def project(normed, weight, bias):
    return jnp.dot(normed, weight, preferred_element_type=jnp.float32) + bias

def attend(query_rows, key_rows, value_rows, visible):
    scores = jnp.dot(query_rows, key_rows.T, preferred_element_type=jnp.float32) * HEAD ** (-0.5)
    scores = jnp.where(visible, scores, MASKED)
    highest = lax.optimization_barrier(jnp.max(scores, axis=-1, keepdims=True))
    weights = jnp.where(visible, jnp.exp(scores - highest), 0.0)
    totals = lax.optimization_barrier(jnp.sum(weights, axis=-1, keepdims=True))
    blended = jnp.dot(weights.astype(jnp.bfloat16), value_rows, preferred_element_type=jnp.float32)
    return (blended / totals).astype(jnp.bfloat16)

def attend_decode(query_rows, key_rows, value_rows, prefix_visible, own_keys, own_values, own_visible):
    factor = HEAD ** (-0.5)
    far_scores = jnp.dot(query_rows, key_rows.T, preferred_element_type=jnp.float32) * factor
    far_scores = jnp.where(prefix_visible, far_scores, MASKED)
    near_scores = jnp.einsum('sd,std->st', query_rows.astype(jnp.float32), own_keys.astype(jnp.float32)) * factor
    near_scores = jnp.where(own_visible[None, :], near_scores, MASKED)
    highest = jnp.maximum(lax.optimization_barrier(jnp.max(far_scores, axis=-1)), lax.optimization_barrier(jnp.max(near_scores, axis=-1)))[:, None]
    far_weights = jnp.where(prefix_visible, jnp.exp(far_scores - highest), 0.0)
    near_weights = jnp.where(own_visible[None, :], jnp.exp(near_scores - highest), 0.0)
    totals = lax.optimization_barrier(jnp.sum(far_weights, axis=-1)) + lax.optimization_barrier(jnp.sum(near_weights, axis=-1))
    near_rounded = lax.optimization_barrier(near_weights.astype(jnp.bfloat16))
    blended = jnp.dot(far_weights.astype(jnp.bfloat16), value_rows, preferred_element_type=jnp.float32)
    blended = blended + jnp.einsum('st,std->sd', near_rounded.astype(jnp.float32), own_values.astype(jnp.float32))
    return (blended / totals[:, None]).astype(jnp.bfloat16)

def reference(span_rows, step_rows, lengths, sample_prompt, norm_gain, query_weight, key_weight, value_weight, query_bias, key_bias, value_bias, out_weight, cache_keys, cache_values):
    kv_group = HEADS // KV_HEADS
    positions_all = PREFIX + SPAN
    normed = norm_rows(span_rows, norm_gain)
    span_places = PREFIX + jnp.arange(SPAN, dtype=jnp.int32)
    grid_places = jnp.broadcast_to(span_places, (PROMPTS, SPAN))
    queries = rotate(project(normed, query_weight, query_bias).reshape(PROMPTS, SPAN, HEADS, HEAD), grid_places).astype(jnp.bfloat16)
    new_keys = rotate(project(normed, key_weight, key_bias).reshape(PROMPTS, SPAN, KV_HEADS, HEAD), grid_places).astype(jnp.bfloat16)
    new_values = project(normed, value_weight, value_bias).astype(jnp.bfloat16).reshape(PROMPTS, SPAN, KV_HEADS, HEAD)
    all_keys = jnp.concatenate([cache_keys.reshape(PROMPTS, PREFIX, KV_HEADS, HEAD), new_keys], axis=1)
    all_values = jnp.concatenate([cache_values.reshape(PROMPTS, PREFIX, KV_HEADS, HEAD), new_values], axis=1)
    key_places = jnp.arange(positions_all, dtype=jnp.int32)
    head_ids = jnp.arange(HEADS, dtype=jnp.int32)
    span_parts = []
    for prompt in range(PROMPTS):
        visible = (key_places[None, :] < lengths[prompt]) & (key_places[None, :] <= span_places[:, None])
        prompt_queries = queries[prompt]
        prompt_keys = all_keys[prompt]
        prompt_values = all_values[prompt]

        def one_head(head_index):
            kv_index = head_index // kv_group
            query_rows = lax.dynamic_index_in_dim(prompt_queries, head_index, 1, keepdims=False)
            key_rows = lax.dynamic_index_in_dim(prompt_keys, kv_index, 1, keepdims=False)
            value_rows = lax.dynamic_index_in_dim(prompt_values, kv_index, 1, keepdims=False)
            return attend(query_rows, key_rows, value_rows, visible)
        per_head = lax.map(one_head, head_ids)
        span_parts.append(jnp.transpose(per_head, (1, 0, 2)).reshape(SPAN, HEADS * HEAD))
    span_attention = jnp.stack(span_parts)
    span_out = jnp.dot(span_attention, out_weight, preferred_element_type=jnp.float32).astype(jnp.bfloat16)
    length_of = lengths[sample_prompt]
    prompt_ids = jnp.arange(PROMPTS, dtype=jnp.int32)
    prefix_visible = ((sample_prompt[:, None, None] == prompt_ids[None, :, None]) & (key_places[None, None, :] < length_of[:, None, None])).reshape(SAMPLES, PROMPTS * positions_all)
    flat_keys = all_keys.reshape(PROMPTS * positions_all, KV_HEADS, HEAD)
    flat_values = all_values.reshape(PROMPTS * positions_all, KV_HEADS, HEAD)
    made_keys = jnp.zeros((SAMPLES, STEPS, KV_HEADS, HEAD), jnp.bfloat16)
    made_values = jnp.zeros((SAMPLES, STEPS, KV_HEADS, HEAD), jnp.bfloat16)
    step_ids = jnp.arange(STEPS, dtype=jnp.int32)
    results = []
    for step_index in range(STEPS):
        normed_step = norm_rows(step_rows[step_index], norm_gain)
        places_now = length_of + step_index
        step_queries = rotate(project(normed_step, query_weight, query_bias).reshape(SAMPLES, HEADS, HEAD), places_now).astype(jnp.bfloat16)
        fresh_keys = rotate(project(normed_step, key_weight, key_bias).reshape(SAMPLES, KV_HEADS, HEAD), places_now).astype(jnp.bfloat16)
        fresh_values = project(normed_step, value_weight, value_bias).astype(jnp.bfloat16).reshape(SAMPLES, KV_HEADS, HEAD)
        made_keys = made_keys.at[:, step_index].set(fresh_keys)
        made_values = made_values.at[:, step_index].set(fresh_values)
        own_visible = step_ids <= step_index
        current_keys = made_keys
        current_values = made_values

        def decode_head(head_index):
            kv_index = head_index // kv_group
            query_rows = lax.dynamic_index_in_dim(step_queries, head_index, 1, keepdims=False)
            key_rows = lax.dynamic_index_in_dim(flat_keys, kv_index, 1, keepdims=False)
            value_rows = lax.dynamic_index_in_dim(flat_values, kv_index, 1, keepdims=False)
            own_keys = lax.dynamic_index_in_dim(current_keys, kv_index, 2, keepdims=False)
            own_values = lax.dynamic_index_in_dim(current_values, kv_index, 2, keepdims=False)
            return attend_decode(query_rows, key_rows, value_rows, prefix_visible, own_keys, own_values, own_visible)
        per_head = lax.map(decode_head, head_ids)
        step_attention = jnp.transpose(per_head, (1, 0, 2)).reshape(SAMPLES, HEADS * HEAD)
        results.append(jnp.dot(step_attention, out_weight, preferred_element_type=jnp.float32).astype(jnp.bfloat16))
    return (span_out, jnp.stack(results))
```

```python
import functools
import math

import jax
import jax.numpy as jnp
from jax import lax
from jax.experimental import pallas as pl
from jax.experimental.pallas import tpu as pltpu
from jax.sharding import PartitionSpec as P

HEADS = 28
KV_HEADS = 4
HEAD = 128


ROPE_BASE = 1000000.0
NORM_EPS = 1e-06
MASKED = -1e30


def norm_rows(inputs, norm_gain):
    widened = inputs.astype(jnp.float32)
    inverse = lax.rsqrt(jnp.mean(widened * widened, axis=-1, keepdims=True) + NORM_EPS)
    return (widened * inverse * norm_gain).astype(jnp.bfloat16)


def rotate(vectors, positions):
    width = vectors.shape[-1]
    half = width // 2
    exponent = jnp.arange(half, dtype=jnp.float32) * (2.0 / width)
    frequency = jnp.exp(exponent * -math.log(ROPE_BASE))
    angles = positions.astype(jnp.float32)[..., None, None] * frequency
    cosine = jnp.cos(angles)
    sine = jnp.sin(angles)
    first = vectors[..., :half]
    second = vectors[..., half:]
    return jnp.concatenate(
        [first * cosine - second * sine, second * cosine + first * sine], axis=-1
    )


def project(normed, weight, bias):
    return jnp.dot(normed, weight, preferred_element_type=jnp.float32) + bias


def key_positions(count, prefix_dev, span_dev, prefix_all):
    row_index = jnp.arange(count, dtype=jnp.int32)
    device = row_index // (prefix_dev + span_dev)
    offset = row_index % (prefix_dev + span_dev)
    return jnp.where(
        offset < prefix_dev,
        device * prefix_dev + offset,
        prefix_all + device * span_dev + offset - prefix_dev,
    )


def local_gathering(
    span_rows,
    step_rows,
    lengths,
    sample_prompt,
    norm_gain,
    query_weight,
    key_weight,
    value_weight,
    query_bias,
    key_bias,
    value_bias,
    out_weight,
    cache_keys,
    cache_values,
):
    cycle_size = lax.axis_size("ctx")
    cycle_place = lax.axis_index("ctx")
    prompt_count = span_rows.shape[0]
    span_dev = span_rows.shape[1]
    prefix_dev = cache_keys.shape[1]
    kv_local = key_weight.shape[1] // HEAD
    kv_group = HEADS // KV_HEADS
    heads_local = kv_local * kv_group
    prefix_all = prefix_dev * cycle_size
    factor = HEAD ** (-0.5)
    full_query = lax.all_gather(query_weight, "ctx", axis=0, tiled=True)
    normed = norm_rows(span_rows, norm_gain)
    span_places = prefix_all + cycle_place * span_dev + jnp.arange(span_dev, dtype=jnp.int32)
    grid_places = jnp.broadcast_to(span_places, (prompt_count, span_dev))
    queries = rotate(
        project(normed, full_query, query_bias).reshape(prompt_count, span_dev, heads_local, HEAD),
        grid_places,
    ).astype(jnp.bfloat16)
    new_keys = rotate(
        project(normed, key_weight, key_bias).reshape(prompt_count, span_dev, kv_local, HEAD),
        grid_places,
    ).astype(jnp.bfloat16)
    new_values = project(normed, value_weight, value_bias).astype(jnp.bfloat16)
    key_block = jnp.concatenate(
        [cache_keys, new_keys.reshape(prompt_count, span_dev, kv_local * HEAD)], axis=1
    )
    value_block = jnp.concatenate([cache_values, new_values], axis=1)
    query_rows = (
        queries.reshape(prompt_count, span_dev, kv_local, kv_group, HEAD)
        .transpose(0, 2, 1, 3, 4)
        .reshape(prompt_count, kv_local, span_dev * kv_group, HEAD)
    )
    query_places = jnp.repeat(span_places, kv_group)
    row_count = span_dev * kv_group
    highest = jnp.full((prompt_count, kv_local, row_count), MASKED, jnp.float32)
    key_piece = lax.all_gather(key_block, "ctx", axis=1, tiled=True)
    value_piece = lax.all_gather(value_block, "ctx", axis=1, tiled=True)
    count = key_piece.shape[1]
    places = key_positions(count, prefix_dev, span_dev, prefix_all)
    key_grid = key_piece.reshape(prompt_count, count, kv_local, HEAD)
    value_grid = value_piece.reshape(prompt_count, count, kv_local, HEAD)
    scores = (
        jnp.einsum("pgqd,pkgd->pgqk", query_rows, key_grid, preferred_element_type=jnp.float32)
        * factor
    )
    visible = (places[None, None, None, :] < lengths[:, None, None, None]) & (
        places[None, None, None, :] <= query_places[None, None, :, None]
    )
    scores = jnp.where(visible, scores, MASKED)
    raised = jnp.maximum(highest, jnp.max(scores, axis=-1))
    weights = jnp.where(visible, jnp.exp(scores - raised[..., None]), 0.0)
    totals = jnp.sum(weights, axis=-1)
    blended = jnp.einsum(
        "pgqk,pkgd->pgqd",
        weights.astype(jnp.bfloat16),
        value_grid,
        preferred_element_type=jnp.float32,
    )
    highest, totals, blended = (raised, totals, blended)
    key_all, value_all = (
        lax.all_gather(key_block, "ctx", axis=1, tiled=True),
        lax.all_gather(value_block, "ctx", axis=1, tiled=True),
    )
    span_attention = (blended / totals[..., None]).astype(jnp.bfloat16)
    span_attention = (
        span_attention.reshape(prompt_count, kv_local, span_dev, kv_group, HEAD)
        .transpose(0, 2, 1, 3, 4)
        .reshape(prompt_count, span_dev, heads_local * HEAD)
    )
    full_out = lax.all_gather(out_weight, "ctx", axis=1, tiled=True)
    span_terms = jnp.dot(span_attention, full_out, preferred_element_type=jnp.float32)
    span_out = lax.psum_scatter(
        span_terms.astype(jnp.bfloat16), "tp", scatter_dimension=2, tiled=True
    )
    gathered_rows = key_all.shape[1]
    key_grid = key_all.reshape(prompt_count, gathered_rows, kv_local, HEAD)
    value_grid = value_all.reshape(prompt_count, gathered_rows, kv_local, HEAD)
    all_places = key_positions(gathered_rows, prefix_dev, span_dev, prefix_all)
    picked = sample_prompt[:, None] == jnp.arange(prompt_count, dtype=jnp.int32)[None, :]
    length_of = jnp.sum(jnp.where(picked, lengths[None, :], 0), axis=1)
    prefix_visible = picked[:, :, None] & (all_places[None, None, :] < length_of[:, None, None])
    wide_visible = prefix_visible[:, None, None, :, :]
    sample_count = step_rows.shape[1]
    step_count = step_rows.shape[0]
    step_ids = jnp.arange(step_count, dtype=jnp.int32)
    made_keys = jnp.zeros((sample_count, step_count, kv_local, HEAD), jnp.bfloat16)
    made_values = jnp.zeros((sample_count, step_count, kv_local, HEAD), jnp.bfloat16)
    outputs = []
    for step_index in range(step_count):
        normed_step = norm_rows(step_rows[step_index], norm_gain)
        places_now = length_of + step_index
        step_queries = rotate(
            project(normed_step, full_query, query_bias).reshape(sample_count, heads_local, HEAD),
            places_now,
        ).astype(jnp.bfloat16)
        step_queries = step_queries.reshape(sample_count, kv_local, kv_group, HEAD)
        fresh_keys = rotate(
            project(normed_step, key_weight, key_bias).reshape(sample_count, kv_local, HEAD),
            places_now,
        ).astype(jnp.bfloat16)
        fresh_values = (
            project(normed_step, value_weight, value_bias)
            .astype(jnp.bfloat16)
            .reshape(sample_count, kv_local, HEAD)
        )
        made_keys = made_keys.at[:, step_index].set(fresh_keys)
        made_values = made_values.at[:, step_index].set(fresh_values)
        own_visible = step_ids <= step_index
        far_scores = (
            jnp.einsum(
                "sgqd,pkgd->sgqpk", step_queries, key_grid, preferred_element_type=jnp.float32
            )
            * factor
        )
        far_scores = jnp.where(wide_visible, far_scores, MASKED)
        near_scores = (
            jnp.einsum(
                "sgqd,stgd->sgqt", step_queries, made_keys, preferred_element_type=jnp.float32
            )
            * factor
        )
        near_scores = jnp.where(own_visible, near_scores, MASKED)
        highest_now = jnp.maximum(jnp.max(far_scores, axis=(3, 4)), jnp.max(near_scores, axis=-1))
        far_weights = jnp.where(
            wide_visible, jnp.exp(far_scores - highest_now[..., None, None]), 0.0
        )
        near_weights = jnp.where(own_visible, jnp.exp(near_scores - highest_now[..., None]), 0.0)
        totals_now = jnp.sum(far_weights, axis=(3, 4)) + jnp.sum(near_weights, axis=-1)
        blended_now = jnp.einsum(
            "sgqpk,pkgd->sgqd",
            far_weights.astype(jnp.bfloat16),
            value_grid,
            preferred_element_type=jnp.float32,
        )
        blended_now = blended_now + jnp.einsum(
            "sgqt,stgd->sgqd",
            near_weights.astype(jnp.bfloat16),
            made_values,
            preferred_element_type=jnp.float32,
        )
        step_attention = (
            (blended_now / totals_now[..., None])
            .astype(jnp.bfloat16)
            .reshape(sample_count, heads_local * HEAD)
        )
        outputs.append(step_attention)
    stacked = jnp.stack(outputs)
    decode_terms = jnp.dot(stacked, full_out, preferred_element_type=jnp.float32)
    dec_out = lax.psum_scatter(
        decode_terms.astype(jnp.bfloat16), "tp", scatter_dimension=2, tiled=True
    )
    return (span_out, dec_out)


LOG2_E = 1.4426950408889634
VMEM = pl.BlockSpec(memory_space=pltpu.VMEM)
SMEM = pl.BlockSpec(memory_space=pltpu.SMEM)


def rotation_tables(positions):
    half = HEAD // 2
    exponent = jnp.arange(half, dtype=jnp.float32) * (2.0 / HEAD)
    frequency = jnp.exp(exponent * -math.log(ROPE_BASE))
    angles = positions.astype(jnp.float32)[:, None] * frequency
    cosine = jnp.cos(angles)
    sine = jnp.sin(angles)
    return (
        jnp.concatenate([cosine, cosine], axis=-1),
        jnp.concatenate([-sine, sine], axis=-1),
    )


def rotate_block(block, cosine, sine):
    return block * cosine + pltpu.roll(block, HEAD // 2, 1) * sine


def norm_kernel(place_ref, span_ref, step_ref, gain_ref, normed_ref, *rest):
    message_refs, widened = rest[:-1], rest[-1]
    prompts, span_dev, _ = span_ref.shape
    steps, samples, _ = step_ref.shape
    for prompt in range(prompts):
        widened[prompt * span_dev : (prompt + 1) * span_dev, :] = span_ref[prompt].astype(
            jnp.float32
        )
    base = prompts * span_dev
    for step in range(steps):
        widened[base + step * samples : base + (step + 1) * samples, :] = step_ref[step].astype(
            jnp.float32
        )
    rows = widened[...]
    inverse = lax.rsqrt(jnp.mean(rows * rows, axis=-1, keepdims=True) + NORM_EPS)
    normed_ref[...] = (rows * inverse * gain_ref[...]).astype(jnp.bfloat16)
    width = message_refs[0].shape[1]
    for slot, message_ref in enumerate(message_refs):
        start = pl.multiple_of((place_ref[0] ^ slot) * width, width)
        message_ref[...] = normed_ref[:, pl.ds(start, width)]


def key_value_kernel(
    normed_ref,
    key_weight_ref,
    value_weight_ref,
    key_bias_ref,
    value_bias_ref,
    cosine_ref,
    sine_ref,
    cache_keys_ref,
    cache_values_ref,
    packed_ref,
    own_ref,
):
    prompts, prefix_dev, width = cache_keys_ref.shape
    own_rows = own_ref.shape[1]
    span_dev = (normed_ref.shape[0] - own_rows) // prompts
    block = prefix_dev + span_dev
    normed = normed_ref[...]
    keys = (
        jnp.dot(normed, key_weight_ref[...], preferred_element_type=jnp.float32)
        + key_bias_ref[...]
    )
    values = (
        jnp.dot(normed, value_weight_ref[...], preferred_element_type=jnp.float32)
        + value_bias_ref[...]
    ).astype(jnp.bfloat16)
    cosine, sine = cosine_ref[...], sine_ref[...]
    keys = jnp.concatenate(
        [
            rotate_block(keys[:, at : at + HEAD], cosine, sine)
            for at in range(0, width, HEAD)
        ],
        axis=1,
    ).astype(jnp.bfloat16)
    for kind, (cache_ref, fresh) in enumerate(
        ((cache_keys_ref, keys), (cache_values_ref, values))
    ):
        for prompt in range(prompts):
            start = (kind * prompts + prompt) * block
            packed_ref[start : start + prefix_dev, :] = cache_ref[prompt]
            packed_ref[start + prefix_dev : start + block, :] = fresh[
                prompt * span_dev : (prompt + 1) * span_dev
            ]
        own_ref[kind] = fresh[prompts * span_dev :]


def attend_kernel(
    steps,
    span_start_ref,
    lengths_ref,
    sample_prompt_ref,
    bias_ref,
    cosine_ref,
    sine_ref,
    places_ref,
    own_ref,
    *rest,
):
    *query_refs, near_ref, far_ref, out_ref, rotated = rest
    packed_refs = (near_ref, far_ref)
    prompts = lengths_ref.shape[0]
    samples = sample_prompt_ref.shape[0]
    own_rows = steps * samples
    row_count, columns = out_ref.shape
    span_dev = (row_count - own_rows) // prompts
    kv_width = own_ref.shape[2]
    kv_local = kv_width // HEAD
    heads_local = columns // HEAD
    group = heads_local // kv_local
    scale = HEAD ** (-0.5) * LOG2_E
    cosine, sine = cosine_ref[...], sine_ref[...]
    for head in range(heads_local):
        span = slice(head * HEAD, (head + 1) * HEAD)
        total = query_refs[0][:, span].astype(jnp.float32)
        for query_ref in query_refs[1:]:
            total = total + query_ref[:, span].astype(jnp.float32)
        total = total + bias_ref[:, span]
        rotated[:, span] = rotate_block(total, cosine, sine).astype(jnp.bfloat16)
    places = places_ref[...]
    block = packed_refs[0].shape[1] // (2 * prompts)

    def rows_of(start, count, first_head):
        return jnp.concatenate(
            [
                rotated[start : start + count, head * HEAD : (head + 1) * HEAD]
                for head in range(first_head, first_head + group)
            ],
            axis=0,
        )

    def cached(kind, prompt, group_index):
        start = (kind * prompts + prompt) * block
        lanes = slice(group_index * HEAD, (group_index + 1) * HEAD)
        return jnp.concatenate(
            [
                packed_ref[index, start : start + block, lanes]
                for packed_ref in packed_refs
                for index in range(packed_ref.shape[0])
            ],
            axis=0,
        )

    def score(queries, keys, visible):
        raw = lax.dot_general(
            queries, keys, (((1,), (1,)), ((), ())), preferred_element_type=jnp.float32
        )
        return jnp.where(visible, raw * scale, MASKED)

    def store(start, count, first_head, blended):
        for offset in range(group):
            head = first_head + offset
            out_ref[start : start + count, head * HEAD : (head + 1) * HEAD] = blended[
                offset * count : (offset + 1) * count
            ]

    for group_index in range(kv_local):
        first_head = group_index * group
        keys = [cached(0, prompt, group_index) for prompt in range(prompts)]
        values = [cached(1, prompt, group_index) for prompt in range(prompts)]
        row_index = lax.broadcasted_iota(jnp.int32, (group * span_dev, 1), 0)
        query_places = span_start_ref[0] + lax.rem(row_index, span_dev)
        for prompt in range(prompts):
            queries = rows_of(prompt * span_dev, span_dev, first_head)
            limit = jnp.minimum(query_places, lengths_ref[prompt] - 1)
            scores = score(queries, keys[prompt], places <= limit)
            highest = jnp.max(scores, axis=-1, keepdims=True)
            weights = jnp.exp2(scores - highest)
            totals = jnp.sum(weights, axis=-1, keepdims=True)
            blended = jnp.dot(
                weights.astype(jnp.bfloat16), values[prompt], preferred_element_type=jnp.float32
            )
            store(
                prompt * span_dev, span_dev, first_head, (blended / totals).astype(jnp.bfloat16)
            )
        start = prompts * span_dev
        queries = rows_of(start, own_rows, first_head)
        row_index = lax.rem(lax.broadcasted_iota(jnp.int32, (group * own_rows, 1), 0), own_rows)
        sample = lax.rem(row_index, samples)
        step = lax.div(row_index, samples)
        own_index = lax.broadcasted_iota(jnp.int32, (1, own_rows), 1)
        own_visible = (lax.rem(own_index, samples) == sample) & (
            lax.div(own_index, samples) <= step
        )
        own_lanes = slice(group_index * HEAD, (group_index + 1) * HEAD)
        parts = [score(queries, own_ref[0, :, own_lanes], own_visible)]
        for prompt in range(prompts):
            limit = jnp.full(row_index.shape, -1, jnp.int32)
            for index in range(samples):
                reach = jnp.where(
                    sample_prompt_ref[index] == prompt, lengths_ref[prompt] - 1, -1
                )
                limit = jnp.where(sample == index, reach, limit)
            parts.append(score(queries, keys[prompt], places <= limit))
        highest = functools.reduce(
            jnp.maximum, [jnp.max(part, axis=-1, keepdims=True) for part in parts]
        )
        weights = [jnp.exp2(part - highest) for part in parts]
        totals = sum(jnp.sum(weight, axis=-1, keepdims=True) for weight in weights)
        blended = sum(
            jnp.dot(weight.astype(jnp.bfloat16), value, preferred_element_type=jnp.float32)
            for weight, value in zip(weights, [own_ref[1, :, own_lanes]] + values)
        )
        store(start, own_rows, first_head, (blended / totals).astype(jnp.bfloat16))


def both_cores(block, is_second, pairs):
    other = lax.ppermute(block, "ctx", pairs)
    return jnp.where(
        is_second, jnp.concatenate([other, block]), jnp.concatenate([block, other])
    )


def local_moving_rows(
    span_rows,
    step_rows,
    lengths,
    sample_prompt,
    norm_gain,
    query_weight,
    key_weight,
    value_weight,
    query_bias,
    key_bias,
    value_bias,
    out_weight,
    cache_keys,
    cache_values,
):
    ctx_size = lax.axis_size("ctx")
    tp_size = lax.axis_size("tp")
    ctx_place = lax.axis_index("ctx")
    tp_place = lax.axis_index("tp")
    chip_place, core_place = ctx_place // 2, ctx_place % 2
    chips = ctx_size // 2
    prompts, span_dev, model = span_rows.shape
    steps, samples, _ = step_rows.shape
    prefix_dev, kv_width = cache_keys.shape[1:]
    prefix_all = prefix_dev * ctx_size
    columns = query_weight.shape[1]
    row_count = prompts * span_dev + steps * samples
    chip_width = model // chips
    core_pairs = [(place, place ^ 1) for place in range(ctx_size)]

    def to_chip(block, slot):
        return lax.ppermute(
            block, "ctx", [(place, place ^ (2 * slot)) for place in range(ctx_size)]
        )

    bf16 = functools.partial(jax.ShapeDtypeStruct, dtype=jnp.bfloat16)
    normed, *messages = pl.pallas_call(
        norm_kernel,
        out_shape=[bf16((row_count, model))] + [bf16((row_count, chip_width))] * chips,
        in_specs=[SMEM, VMEM, VMEM, VMEM],
        out_specs=[VMEM] * (1 + chips),
        scratch_shapes=[pltpu.VMEM((row_count, model), jnp.float32)],
        name="norm",
    )(chip_place.reshape(1), span_rows, step_rows, norm_gain.reshape(1, model))
    inbound = [messages[0]] + [to_chip(messages[slot], slot) for slot in range(1, chips)]
    chip_query = both_cores(query_weight, core_place == 1, core_pairs)

    span_places = prefix_all + ctx_place * span_dev + jnp.arange(span_dev, dtype=jnp.int32)
    picked = sample_prompt[:, None] == jnp.arange(prompts, dtype=jnp.int32)[None, :]
    length_of = jnp.sum(jnp.where(picked, lengths[None, :], 0), axis=1)
    step_places = jnp.arange(steps, dtype=jnp.int32)[:, None] + length_of[None, :]
    row_places = jnp.concatenate(
        [jnp.tile(span_places, prompts), step_places.reshape(steps * samples)]
    )
    cosine, sine = rotation_tables(row_places)
    block = prefix_dev + span_dev
    packed, own = pl.pallas_call(
        key_value_kernel,
        out_shape=[
            bf16((2 * prompts * block, kv_width)),
            bf16((2, steps * samples, kv_width)),
        ],
        in_specs=[VMEM] * 9,
        out_specs=[VMEM] * 2,
        name="key_value",
    )(
        normed,
        key_weight,
        value_weight,
        key_bias.reshape(1, kv_width),
        value_bias.reshape(1, kv_width),
        cosine,
        sine,
        cache_keys,
        cache_values,
    )
    near_packed = jnp.stack([packed] + [to_chip(packed, slot) for slot in range(1, chips)])
    far_packed = lax.ppermute(near_packed, "ctx", core_pairs)

    partial = [
        jnp.dot(rows, chip_query, preferred_element_type=jnp.float32) for rows in inbound
    ]
    shares = [partial[0]] + [
        to_chip(partial[slot].astype(jnp.bfloat16), slot) for slot in range(1, chips)
    ]

    slot_chips = chip_place ^ jnp.arange(chips, dtype=jnp.int32)
    owners = jnp.concatenate([2 * slot_chips + core_place, 2 * slot_chips + 1 - core_place])
    offsets = jnp.arange(block, dtype=jnp.int32)
    places = jnp.where(
        offsets < prefix_dev,
        owners[:, None] * prefix_dev + offsets,
        prefix_all + owners[:, None] * span_dev + offsets - prefix_dev,
    ).reshape(1, ctx_size * block)
    attention = pl.pallas_call(
        functools.partial(attend_kernel, steps),
        out_shape=bf16((row_count, columns)),
        in_specs=[SMEM] * 3 + [VMEM] * (5 + chips + 2),
        out_specs=VMEM,
        scratch_shapes=[pltpu.VMEM((row_count, columns), jnp.bfloat16)],
        name="attend",
    )(
        (prefix_all + ctx_place * span_dev).reshape(1),
        lengths,
        sample_prompt,
        query_bias.reshape(1, columns),
        cosine,
        sine,
        places,
        own,
        *shares,
        near_packed,
        far_packed,
    )

    chip_out = both_cores(out_weight.T, core_place == 1, core_pairs)
    attended = [attention] + [to_chip(attention, slot) for slot in range(1, chips)]
    terms = [
        lax.dot_general(
            rows, chip_out, (((1,), (1,)), ((), ())), preferred_element_type=jnp.float32
        ).astype(jnp.bfloat16)
        for rows in attended
    ]
    returned = jnp.stack(
        [terms[0]] + [to_chip(terms[slot], slot) for slot in range(1, chips)]
    )
    mine = lax.dynamic_index_in_dim(returned, tp_place ^ chip_place, 0, keepdims=False)
    total = mine.astype(jnp.float32)
    for slot in range(1, tp_size):
        leaving = lax.dynamic_index_in_dim(
            returned, tp_place ^ slot ^ chip_place, 0, keepdims=False
        )
        arriving = lax.ppermute(
            leaving, "tp", [(place, place ^ slot) for place in range(tp_size)]
        )
        total = total + arriving.astype(jnp.float32)
    outcome = total.astype(jnp.bfloat16)
    span_count = prompts * span_dev
    return (
        outcome[:span_count].reshape(prompts, span_dev, -1),
        outcome[span_count:].reshape(steps, samples, -1),
    )


def rows_are_lighter(mesh, rows, model):
    ctx_size, tp_size = mesh.shape["ctx"], mesh.shape["tp"]
    fits = ctx_size == 2 * tp_size and tp_size & (tp_size - 1) == 0
    return fits and rows < model


def solution(mesh):
    def local(span_rows, step_rows, lengths, sample_prompt, norm_gain, query_weight, *others):
        whole_rows = (span_rows.shape[0] * span_rows.shape[1], step_rows.shape[0] * step_rows.shape[1])
        rows = sum(whole_rows) * mesh.shape["ctx"]
        form = local_gathering
        if rows_are_lighter(mesh, rows, query_weight.shape[0] * mesh.shape["ctx"]):
            form = local_moving_rows
        return form(
            span_rows, step_rows, lengths, sample_prompt, norm_gain, query_weight, *others
        )

    return jax.shard_map(
        local,
        mesh=mesh,
        in_specs=(
            P(None, "ctx", None),
            P(None, "ctx", None),
            P(),
            P("ctx"),
            P(),
            P("ctx", "tp"),
            P(None, "tp"),
            P(None, "tp"),
            P("tp"),
            P("tp"),
            P("tp"),
            P("tp", "ctx"),
            P(None, "ctx", "tp"),
            P(None, "ctx", "tp"),
        ),
        out_specs=(P(None, "ctx", "tp"), P(None, "ctx", "tp")),
        check_vma=False,
    )
```

```python
import functools
import math

import jax
import jax.numpy as jnp
from jax import lax
from jax.experimental import pallas as pl
from jax.experimental.pallas import tpu as pltpu
from jax.sharding import PartitionSpec as P


HEADS = 28
KV_HEADS = 4
HEAD = 128


ROPE_BASE = 1000000.0
NORM_EPS = 1e-06
MASKED = -1e30


def norm_rows(inputs, norm_gain):
    widened = inputs.astype(jnp.float32)
    inverse = lax.rsqrt(jnp.mean(widened * widened, axis=-1, keepdims=True) + NORM_EPS)
    return (widened * inverse * norm_gain).astype(jnp.bfloat16)


def rotate(vectors, positions):
    width = vectors.shape[-1]
    half = width // 2
    exponent = jnp.arange(half, dtype=jnp.float32) * (2.0 / width)
    frequency = jnp.exp(exponent * -math.log(ROPE_BASE))
    angles = positions.astype(jnp.float32)[..., None, None] * frequency
    cosine = jnp.cos(angles)
    sine = jnp.sin(angles)
    first = vectors[..., :half]
    second = vectors[..., half:]
    return jnp.concatenate(
        [first * cosine - second * sine, second * cosine + first * sine], axis=-1
    )


def project(normed, weight, bias):
    return jnp.dot(normed, weight, preferred_element_type=jnp.float32) + bias


def key_positions(count, prefix_dev, span_dev, prefix_all):
    row_index = jnp.arange(count, dtype=jnp.int32)
    device = row_index // (prefix_dev + span_dev)
    offset = row_index % (prefix_dev + span_dev)
    return jnp.where(
        offset < prefix_dev,
        device * prefix_dev + offset,
        prefix_all + device * span_dev + offset - prefix_dev,
    )


def local_gathering(
    span_rows,
    step_rows,
    lengths,
    sample_prompt,
    norm_gain,
    query_weight,
    key_weight,
    value_weight,
    query_bias,
    key_bias,
    value_bias,
    out_weight,
    cache_keys,
    cache_values,
):
    cycle_size = lax.axis_size("ctx")
    cycle_place = lax.axis_index("ctx")
    prompt_count = span_rows.shape[0]
    span_dev = span_rows.shape[1]
    prefix_dev = cache_keys.shape[1]
    kv_local = key_weight.shape[1] // HEAD
    kv_group = HEADS // KV_HEADS
    heads_local = kv_local * kv_group
    prefix_all = prefix_dev * cycle_size
    factor = HEAD ** (-0.5)
    full_query = lax.all_gather(query_weight, "ctx", axis=0, tiled=True)
    normed = norm_rows(span_rows, norm_gain)
    span_places = prefix_all + cycle_place * span_dev + jnp.arange(span_dev, dtype=jnp.int32)
    grid_places = jnp.broadcast_to(span_places, (prompt_count, span_dev))
    queries = rotate(
        project(normed, full_query, query_bias).reshape(prompt_count, span_dev, heads_local, HEAD),
        grid_places,
    ).astype(jnp.bfloat16)
    new_keys = rotate(
        project(normed, key_weight, key_bias).reshape(prompt_count, span_dev, kv_local, HEAD),
        grid_places,
    ).astype(jnp.bfloat16)
    new_values = project(normed, value_weight, value_bias).astype(jnp.bfloat16)
    key_block = jnp.concatenate(
        [cache_keys, new_keys.reshape(prompt_count, span_dev, kv_local * HEAD)], axis=1
    )
    value_block = jnp.concatenate([cache_values, new_values], axis=1)
    query_rows = (
        queries.reshape(prompt_count, span_dev, kv_local, kv_group, HEAD)
        .transpose(0, 2, 1, 3, 4)
        .reshape(prompt_count, kv_local, span_dev * kv_group, HEAD)
    )
    query_places = jnp.repeat(span_places, kv_group)
    row_count = span_dev * kv_group
    highest = jnp.full((prompt_count, kv_local, row_count), MASKED, jnp.float32)
    key_piece = lax.all_gather(key_block, "ctx", axis=1, tiled=True)
    value_piece = lax.all_gather(value_block, "ctx", axis=1, tiled=True)
    count = key_piece.shape[1]
    places = key_positions(count, prefix_dev, span_dev, prefix_all)
    key_grid = key_piece.reshape(prompt_count, count, kv_local, HEAD)
    value_grid = value_piece.reshape(prompt_count, count, kv_local, HEAD)
    scores = (
        jnp.einsum("pgqd,pkgd->pgqk", query_rows, key_grid, preferred_element_type=jnp.float32)
        * factor
    )
    visible = (places[None, None, None, :] < lengths[:, None, None, None]) & (
        places[None, None, None, :] <= query_places[None, None, :, None]
    )
    scores = jnp.where(visible, scores, MASKED)
    raised = jnp.maximum(highest, jnp.max(scores, axis=-1))
    weights = jnp.where(visible, jnp.exp(scores - raised[..., None]), 0.0)
    totals = jnp.sum(weights, axis=-1)
    blended = jnp.einsum(
        "pgqk,pkgd->pgqd",
        weights.astype(jnp.bfloat16),
        value_grid,
        preferred_element_type=jnp.float32,
    )
    highest, totals, blended = (raised, totals, blended)
    key_all, value_all = (
        lax.all_gather(key_block, "ctx", axis=1, tiled=True),
        lax.all_gather(value_block, "ctx", axis=1, tiled=True),
    )
    span_attention = (blended / totals[..., None]).astype(jnp.bfloat16)
    span_attention = (
        span_attention.reshape(prompt_count, kv_local, span_dev, kv_group, HEAD)
        .transpose(0, 2, 1, 3, 4)
        .reshape(prompt_count, span_dev, heads_local * HEAD)
    )
    full_out = lax.all_gather(out_weight, "ctx", axis=1, tiled=True)
    span_terms = jnp.dot(span_attention, full_out, preferred_element_type=jnp.float32)
    span_out = lax.psum_scatter(
        span_terms.astype(jnp.bfloat16), "tp", scatter_dimension=2, tiled=True
    )
    gathered_rows = key_all.shape[1]
    key_grid = key_all.reshape(prompt_count, gathered_rows, kv_local, HEAD)
    value_grid = value_all.reshape(prompt_count, gathered_rows, kv_local, HEAD)
    all_places = key_positions(gathered_rows, prefix_dev, span_dev, prefix_all)
    picked = sample_prompt[:, None] == jnp.arange(prompt_count, dtype=jnp.int32)[None, :]
    length_of = jnp.sum(jnp.where(picked, lengths[None, :], 0), axis=1)
    prefix_visible = picked[:, :, None] & (all_places[None, None, :] < length_of[:, None, None])
    wide_visible = prefix_visible[:, None, None, :, :]
    sample_count = step_rows.shape[1]
    step_count = step_rows.shape[0]
    step_ids = jnp.arange(step_count, dtype=jnp.int32)
    made_keys = jnp.zeros((sample_count, step_count, kv_local, HEAD), jnp.bfloat16)
    made_values = jnp.zeros((sample_count, step_count, kv_local, HEAD), jnp.bfloat16)
    outputs = []
    for step_index in range(step_count):
        normed_step = norm_rows(step_rows[step_index], norm_gain)
        places_now = length_of + step_index
        step_queries = rotate(
            project(normed_step, full_query, query_bias).reshape(sample_count, heads_local, HEAD),
            places_now,
        ).astype(jnp.bfloat16)
        step_queries = step_queries.reshape(sample_count, kv_local, kv_group, HEAD)
        fresh_keys = rotate(
            project(normed_step, key_weight, key_bias).reshape(sample_count, kv_local, HEAD),
            places_now,
        ).astype(jnp.bfloat16)
        fresh_values = (
            project(normed_step, value_weight, value_bias)
            .astype(jnp.bfloat16)
            .reshape(sample_count, kv_local, HEAD)
        )
        made_keys = made_keys.at[:, step_index].set(fresh_keys)
        made_values = made_values.at[:, step_index].set(fresh_values)
        own_visible = step_ids <= step_index
        far_scores = (
            jnp.einsum(
                "sgqd,pkgd->sgqpk", step_queries, key_grid, preferred_element_type=jnp.float32
            )
            * factor
        )
        far_scores = jnp.where(wide_visible, far_scores, MASKED)
        near_scores = (
            jnp.einsum(
                "sgqd,stgd->sgqt", step_queries, made_keys, preferred_element_type=jnp.float32
            )
            * factor
        )
        near_scores = jnp.where(own_visible, near_scores, MASKED)
        highest_now = jnp.maximum(jnp.max(far_scores, axis=(3, 4)), jnp.max(near_scores, axis=-1))
        far_weights = jnp.where(
            wide_visible, jnp.exp(far_scores - highest_now[..., None, None]), 0.0
        )
        near_weights = jnp.where(own_visible, jnp.exp(near_scores - highest_now[..., None]), 0.0)
        totals_now = jnp.sum(far_weights, axis=(3, 4)) + jnp.sum(near_weights, axis=-1)
        blended_now = jnp.einsum(
            "sgqpk,pkgd->sgqd",
            far_weights.astype(jnp.bfloat16),
            value_grid,
            preferred_element_type=jnp.float32,
        )
        blended_now = blended_now + jnp.einsum(
            "sgqt,stgd->sgqd",
            near_weights.astype(jnp.bfloat16),
            made_values,
            preferred_element_type=jnp.float32,
        )
        step_attention = (
            (blended_now / totals_now[..., None])
            .astype(jnp.bfloat16)
            .reshape(sample_count, heads_local * HEAD)
        )
        outputs.append(step_attention)
    stacked = jnp.stack(outputs)
    decode_terms = jnp.dot(stacked, full_out, preferred_element_type=jnp.float32)
    dec_out = lax.psum_scatter(
        decode_terms.astype(jnp.bfloat16), "tp", scatter_dimension=2, tiled=True
    )
    return (span_out, dec_out)


LOG2_E = 1.4426950408889634
VMEM = pl.BlockSpec(memory_space=pltpu.VMEM)
HBM = pl.BlockSpec(memory_space=pltpu.HBM)
SMEM = pl.BlockSpec(memory_space=pltpu.SMEM)
KERNEL = pltpu.CompilerParams(vmem_limit_bytes=16 * 2**20)
NORM_KERNEL = pltpu.CompilerParams(vmem_limit_bytes=66400000)
KEY_VALUE_KERNEL = pltpu.CompilerParams(vmem_limit_bytes=60 * 2**20)


def rotation_tables(positions):
    half = HEAD // 2
    lane = lax.broadcasted_iota(jnp.int32, (1, HEAD), 1)
    exponent = lax.rem(lane, half).astype(jnp.float32) * (2.0 / HEAD)
    frequency = jnp.exp(exponent * -math.log(ROPE_BASE))
    angles = positions.astype(jnp.float32) * frequency
    sine = jnp.sin(angles)
    return jnp.cos(angles), jnp.where(lane < half, -sine, sine)


def rotate_block(block, cosine, sine):
    return block * cosine + pltpu.roll(block, HEAD // 2, 1) * sine


def fetch_all(sources, targets, semaphores):
    copies = [
        pltpu.make_async_copy(source, target, semaphores.at[index])
        for index, (source, target) in enumerate(zip(sources, targets))
    ]
    for copy in copies:
        copy.start()
    for copy in copies:
        copy.wait()


def norm_kernel(place_ref, span_hbm, step_hbm, gain_hbm, *rest):
    *message_refs, normed_ref, widened, span_ref, step_ref, gain_ref, semaphores = rest
    fetch_all((span_hbm, step_hbm, gain_hbm), (span_ref, step_ref, gain_ref), semaphores)
    prompts, span_dev, _ = span_ref.shape
    steps, samples, _ = step_ref.shape
    for prompt in range(prompts):
        widened[prompt * span_dev : (prompt + 1) * span_dev, :] = span_ref[prompt].astype(
            jnp.float32
        )
    base = prompts * span_dev
    for step in range(steps):
        widened[base + step * samples : base + (step + 1) * samples, :] = step_ref[step].astype(
            jnp.float32
        )
    rows = widened[...]
    inverse = lax.rsqrt(jnp.mean(rows * rows, axis=-1, keepdims=True) + NORM_EPS)
    normed_ref[...] = (rows * inverse * gain_ref[...][None, :]).astype(jnp.bfloat16)
    width = message_refs[0].shape[1]
    for slot, message_ref in enumerate(message_refs):
        start = pl.multiple_of((place_ref[0] ^ slot) * width, width)
        message_ref[...] = normed_ref[:, pl.ds(start, width)]


def key_value_kernel(
    steps,
    ctx_ref,
    lengths_ref,
    sample_prompt_ref,
    *rest,
):
    chips = len(rest) - 16
    message_refs, rest = rest[:chips], rest[chips:]
    (key_weight_hbm, value_weight_hbm, *other_hbm), rest = rest[:6], rest[6:]
    (packed_ref, own_ref, cosine_ref, sine_ref), rest = rest[:4], rest[4:]
    weight_ref, *fetched, semaphores = rest
    key_bias_ref, value_bias_ref, cache_keys_ref, cache_values_ref = fetched[:4]
    prompts, prefix_dev, width = cache_keys_ref.shape
    copies = [
        pltpu.make_async_copy(source, target, semaphores.at[index])
        for index, (source, target) in enumerate(
            [
                (key_weight_hbm, weight_ref.at[:, :width]),
                (value_weight_hbm, weight_ref.at[:, width:]),
            ]
            + list(zip(other_hbm, fetched))
        )
    ]
    for copy in copies:
        copy.start()
    samples = sample_prompt_ref.shape[0]
    own_rows = steps * samples
    row_count, chip_width = message_refs[0].shape
    span_dev = (row_count - own_rows) // prompts
    block = prefix_dev + span_dev
    row_index = lax.broadcasted_iota(jnp.int32, (row_count, 1), 0)
    span_start = (2 * chips * prefix_dev) + ctx_ref[0] * span_dev
    positions = span_start + lax.rem(row_index, span_dev)
    own_index = row_index - prompts * span_dev
    for index in range(samples):
        start = lengths_ref[sample_prompt_ref[index]]
        taken = (own_index >= 0) & (lax.rem(own_index, samples) == index)
        positions = jnp.where(taken, start + lax.div(own_index, samples), positions)
    cosine, sine = rotation_tables(positions)
    cosine_ref[...], sine_ref[...] = cosine, sine
    for copy in copies:
        copy.wait()
    products = None
    for slot, message_ref in enumerate(message_refs):
        start = pl.multiple_of((lax.div(ctx_ref[0], 2) ^ slot) * chip_width, chip_width)
        product = jnp.dot(
            message_ref[...],
            weight_ref[pl.ds(start, chip_width), :],
            preferred_element_type=jnp.float32,
        )
        products = product if products is None else products + product
    keys = products[:, :width] + key_bias_ref[...][None, :]
    values = (products[:, width:] + value_bias_ref[...][None, :]).astype(jnp.bfloat16)
    keys = jnp.concatenate(
        [
            rotate_block(keys[:, at : at + HEAD], cosine, sine)
            for at in range(0, width, HEAD)
        ],
        axis=1,
    ).astype(jnp.bfloat16)
    for kind, (cache_ref, fresh) in enumerate(
        ((cache_keys_ref, keys), (cache_values_ref, values))
    ):
        for prompt in range(prompts):
            start = (kind * prompts + prompt) * block
            packed_ref[start : start + prefix_dev, :] = cache_ref[prompt]
            packed_ref[start + prefix_dev : start + block, :] = fresh[
                prompt * span_dev : (prompt + 1) * span_dev
            ]
        own_ref[kind] = fresh[prompts * span_dev :]


def query_kernel(core_ref, rows_ref, own_ref, other_ref, out_ref):
    half = own_ref.shape[0]

    def product(first_ref, second_ref):
        total = jnp.dot(rows_ref[:, :half], first_ref[...], preferred_element_type=jnp.float32)
        total = total + jnp.dot(
            rows_ref[:, half:], second_ref[...], preferred_element_type=jnp.float32
        )
        out_ref[...] = total.astype(out_ref.dtype)

    @pl.when(core_ref[0] == 0)
    def _():
        product(own_ref, other_ref)

    @pl.when(core_ref[0] == 1)
    def _():
        product(other_ref, own_ref)


def out_kernel(core_ref, rows_ref, own_ref, other_ref, out_ref):
    half = own_ref.shape[0]
    rows = rows_ref[...]

    def product(weight_ref):
        return lax.dot_general(
            rows, weight_ref[...], (((1,), (1,)), ((), ())), preferred_element_type=jnp.float32
        ).astype(out_ref.dtype)

    @pl.when(core_ref[0] == 0)
    def _():
        out_ref[:, :half] = product(own_ref)
        out_ref[:, half:] = product(other_ref)

    @pl.when(core_ref[0] == 1)
    def _():
        out_ref[:, :half] = product(other_ref)
        out_ref[:, half:] = product(own_ref)


def attend_kernel(
    steps,
    prefix_dev,
    ctx_ref,
    lengths_ref,
    sample_prompt_ref,
    bias_ref,
    cosine_ref,
    sine_ref,
    own_ref,
    *rest,
):
    *query_refs, near_ref, far_ref, out_ref, rotated = rest
    packed_refs = (near_ref, far_ref)
    prompts = lengths_ref.shape[0]
    samples = sample_prompt_ref.shape[0]
    own_rows = steps * samples
    row_count, columns = out_ref.shape
    span_dev = (row_count - own_rows) // prompts
    kv_width = own_ref.shape[2]
    kv_local = kv_width // HEAD
    heads_local = columns // HEAD
    group = heads_local // kv_local
    scale = HEAD ** (-0.5) * LOG2_E
    cosine, sine = cosine_ref[...], sine_ref[...]
    for head in range(heads_local):
        span = slice(head * HEAD, (head + 1) * HEAD)
        total = query_refs[0][:, span].astype(jnp.float32)
        for query_ref in query_refs[1:]:
            total = total + query_ref[:, span].astype(jnp.float32)
        total = total + bias_ref[span][None, :]
        rotated[:, span] = rotate_block(total, cosine, sine).astype(jnp.bfloat16)
    chips, packed_rows, _ = near_ref.shape
    block = packed_rows // (2 * prompts)
    prefix_all = 2 * chips * prefix_dev
    key_index = lax.broadcasted_iota(jnp.int32, (1, 2 * chips * block), 1)
    slot, offset = lax.div(key_index, block), lax.rem(key_index, block)
    owner = ctx_ref[0] ^ (2 * lax.rem(slot, chips) + lax.div(slot, chips))
    places = jnp.where(
        offset < prefix_dev,
        owner * prefix_dev + offset,
        prefix_all + owner * span_dev + offset - prefix_dev,
    )

    def rows_of(start, count, first_head):
        return jnp.concatenate(
            [
                rotated[start : start + count, head * HEAD : (head + 1) * HEAD]
                for head in range(first_head, first_head + group)
            ],
            axis=0,
        )

    def cached(kind, prompt, group_index):
        start = (kind * prompts + prompt) * block
        lanes = slice(group_index * HEAD, (group_index + 1) * HEAD)
        return jnp.concatenate(
            [
                packed_ref[index, start : start + block, lanes]
                for packed_ref in packed_refs
                for index in range(packed_ref.shape[0])
            ],
            axis=0,
        )

    def score(queries, keys, visible):
        raw = lax.dot_general(
            queries, keys, (((1,), (1,)), ((), ())), preferred_element_type=jnp.float32
        )
        return jnp.where(visible, raw * scale, MASKED)

    def store(start, count, first_head, blended):
        for offset in range(group):
            head = first_head + offset
            out_ref[start : start + count, head * HEAD : (head + 1) * HEAD] = blended[
                offset * count : (offset + 1) * count
            ]

    for group_index in range(kv_local):
        first_head = group_index * group
        keys = [cached(0, prompt, group_index) for prompt in range(prompts)]
        values = [cached(1, prompt, group_index) for prompt in range(prompts)]
        row_index = lax.broadcasted_iota(jnp.int32, (group * span_dev, 1), 0)
        query_places = prefix_all + ctx_ref[0] * span_dev + lax.rem(row_index, span_dev)
        for prompt in range(prompts):
            queries = rows_of(prompt * span_dev, span_dev, first_head)
            limit = jnp.minimum(query_places, lengths_ref[prompt] - 1)
            scores = score(queries, keys[prompt], places <= limit)
            highest = jnp.max(scores, axis=-1, keepdims=True)
            weights = jnp.exp2(scores - highest)
            totals = jnp.sum(weights, axis=-1, keepdims=True)
            blended = jnp.dot(
                weights.astype(jnp.bfloat16), values[prompt], preferred_element_type=jnp.float32
            )
            store(
                prompt * span_dev, span_dev, first_head, (blended / totals).astype(jnp.bfloat16)
            )
        start = prompts * span_dev
        queries = rows_of(start, own_rows, first_head)
        row_index = lax.rem(lax.broadcasted_iota(jnp.int32, (group * own_rows, 1), 0), own_rows)
        sample = lax.rem(row_index, samples)
        step = lax.div(row_index, samples)
        own_index = lax.broadcasted_iota(jnp.int32, (1, own_rows), 1)
        own_visible = (lax.rem(own_index, samples) == sample) & (
            lax.div(own_index, samples) <= step
        )
        own_lanes = slice(group_index * HEAD, (group_index + 1) * HEAD)
        parts = [score(queries, own_ref[0, :, own_lanes], own_visible)]
        for prompt in range(prompts):
            limit = jnp.full(row_index.shape, -1, jnp.int32)
            for index in range(samples):
                reach = jnp.where(
                    sample_prompt_ref[index] == prompt, lengths_ref[prompt] - 1, -1
                )
                limit = jnp.where(sample == index, reach, limit)
            parts.append(score(queries, keys[prompt], places <= limit))
        highest = functools.reduce(
            jnp.maximum, [jnp.max(part, axis=-1, keepdims=True) for part in parts]
        )
        weights = [jnp.exp2(part - highest) for part in parts]
        totals = sum(jnp.sum(weight, axis=-1, keepdims=True) for weight in weights)
        blended = sum(
            jnp.dot(weight.astype(jnp.bfloat16), value, preferred_element_type=jnp.float32)
            for weight, value in zip(weights, [own_ref[1, :, own_lanes]] + values)
        )
        store(start, own_rows, first_head, (blended / totals).astype(jnp.bfloat16))


def add_kernel(*refs):
    share_refs, span_ref, step_ref = refs[:-2], refs[-2], refs[-1]
    prompts, span_dev, _ = span_ref.shape
    steps, samples, _ = step_ref.shape
    total = share_refs[0][...].astype(jnp.float32)
    for share_ref in share_refs[1:]:
        total = total + share_ref[...].astype(jnp.float32)
    for prompt in range(prompts):
        rows = slice(prompt * span_dev, (prompt + 1) * span_dev)
        span_ref[prompt] = total[rows].astype(jnp.bfloat16)
    for step in range(steps):
        start = prompts * span_dev + step * samples
        step_ref[step] = total[start : start + samples].astype(jnp.bfloat16)


def local_moving_rows(
    span_rows,
    step_rows,
    lengths,
    sample_prompt,
    norm_gain,
    query_weight,
    key_weight,
    value_weight,
    query_bias,
    key_bias,
    value_bias,
    out_weight,
    cache_keys,
    cache_values,
):
    ctx_size = lax.axis_size("ctx")
    tp_size = lax.axis_size("tp")
    ctx_place = lax.axis_index("ctx")
    tp_place = lax.axis_index("tp")
    chip_place, core_place = ctx_place // 2, ctx_place % 2
    chips = ctx_size // 2
    prompts, span_dev, model = span_rows.shape
    steps, samples, _ = step_rows.shape
    prefix_dev, kv_width = cache_keys.shape[1:]
    columns = query_weight.shape[1]
    row_count = prompts * span_dev + steps * samples
    chip_width = model // chips
    core_pairs = [(place, place ^ 1) for place in range(ctx_size)]

    def to_chip(block, slot):
        return lax.ppermute(
            block, "ctx", [(place, place ^ (2 * slot)) for place in range(ctx_size)]
        )

    bf16 = functools.partial(jax.ShapeDtypeStruct, dtype=jnp.bfloat16)
    messages = pl.pallas_call(
        norm_kernel,
        out_shape=[bf16((row_count, chip_width))] * chips,
        in_specs=[SMEM, HBM, HBM, HBM],
        out_specs=[VMEM] * chips,
        scratch_shapes=[
            pltpu.VMEM((row_count, model), jnp.bfloat16),
            pltpu.VMEM((row_count, model), jnp.float32),
            pltpu.VMEM(span_rows.shape, jnp.bfloat16),
            pltpu.VMEM(step_rows.shape, jnp.bfloat16),
            pltpu.VMEM(norm_gain.shape, jnp.float32),
            pltpu.SemaphoreType.DMA((3,)),
        ],
        compiler_params=NORM_KERNEL,
        name="norm",
    )(chip_place.reshape(1), span_rows, step_rows, norm_gain)
    inbound = [messages[0]] + [to_chip(messages[slot], slot) for slot in range(1, chips)]
    other_query = lax.ppermute(query_weight, "ctx", core_pairs)
    other_out = lax.ppermute(out_weight.T, "ctx", core_pairs)
    block = prefix_dev + span_dev
    table = jax.ShapeDtypeStruct((row_count, HEAD), jnp.float32)
    packed, own, cosine, sine = pl.pallas_call(
        functools.partial(key_value_kernel, steps),
        out_shape=[
            bf16((2 * prompts * block, kv_width)),
            bf16((2, steps * samples, kv_width)),
            table,
            table,
        ],
        in_specs=[SMEM] * 3 + [VMEM] * chips + [HBM] * 6,
        out_specs=[VMEM] * 4,
        scratch_shapes=[pltpu.VMEM((model, 2 * kv_width), jnp.bfloat16)]
        + [
            pltpu.VMEM(array.shape, array.dtype)
            for array in (key_bias, value_bias, cache_keys, cache_values)
        ]
        + [pltpu.SemaphoreType.DMA((6,))],
        compiler_params=KEY_VALUE_KERNEL,
        name="key_value",
    )(
        ctx_place.reshape(1),
        lengths,
        sample_prompt,
        *messages,
        key_weight,
        value_weight,
        key_bias,
        value_bias,
        cache_keys,
        cache_values,
    )
    near_packed = jnp.stack([packed] + [to_chip(packed, slot) for slot in range(1, chips)])
    far_packed = lax.ppermute(near_packed, "ctx", core_pairs)

    shares = []
    for slot, rows in enumerate(inbound):
        partial = pl.pallas_call(
            query_kernel,
            out_shape=jax.ShapeDtypeStruct(
                (row_count, columns), jnp.bfloat16 if slot else jnp.float32
            ),
            in_specs=[SMEM] + [VMEM] * 3,
            out_specs=VMEM,
            compiler_params=KERNEL,
            name="query_dot",
        )(core_place.reshape(1), rows, query_weight, other_query)
        if slot:
            partial = to_chip(partial, slot)
        shares.append(partial)

    attention = pl.pallas_call(
        functools.partial(attend_kernel, steps, prefix_dev),
        out_shape=bf16((row_count, columns)),
        in_specs=[SMEM] * 3 + [VMEM] * (4 + chips + 2),
        out_specs=VMEM,
        scratch_shapes=[pltpu.VMEM((row_count, columns), jnp.bfloat16)],
        compiler_params=KERNEL,
        name="attend",
    )(
        ctx_place.reshape(1),
        lengths,
        sample_prompt,
        query_bias,
        cosine,
        sine,
        own,
        *shares,
        near_packed,
        far_packed,
    )

    attended = [attention] + [to_chip(attention, slot) for slot in range(1, chips)]
    returned = []
    for slot, rows in enumerate(attended):
        terms = pl.pallas_call(
            out_kernel,
            out_shape=bf16((row_count, columns)),
            in_specs=[SMEM] + [VMEM] * 3,
            out_specs=VMEM,
            compiler_params=KERNEL,
            name="out_dot",
        )(core_place.reshape(1), rows, out_weight.T, other_out)
        if slot:
            terms = to_chip(terms, slot)
        returned.append(terms)
    returned = jnp.stack(returned)

    def columns_of(slot):
        return lax.dynamic_index_in_dim(returned, tp_place ^ slot ^ chip_place, 0, keepdims=False)

    finals = [columns_of(0)]
    for slot in range(1, tp_size):
        finals.append(
            lax.ppermute(
                columns_of(slot), "tp", [(place, place ^ slot) for place in range(tp_size)]
            )
        )
    return pl.pallas_call(
        add_kernel,
        out_shape=[bf16((prompts, span_dev, columns)), bf16((steps, samples, columns))],
        in_specs=[VMEM] * tp_size,
        out_specs=[VMEM] * 2,
        compiler_params=KERNEL,
        name="add",
    )(*finals)


def rows_are_lighter(mesh, rows, model):
    ctx_size, tp_size = mesh.shape["ctx"], mesh.shape["tp"]
    fits = ctx_size == 2 * tp_size and tp_size & (tp_size - 1) == 0
    return fits and rows < model


def solution(mesh):
    def local(span_rows, step_rows, lengths, sample_prompt, norm_gain, query_weight, *others):
        whole_rows = (span_rows.shape[0] * span_rows.shape[1], step_rows.shape[0] * step_rows.shape[1])
        rows = sum(whole_rows) * mesh.shape["ctx"]
        form = local_gathering
        if rows_are_lighter(mesh, rows, query_weight.shape[0] * mesh.shape["ctx"]):
            form = local_moving_rows
        return form(
            span_rows, step_rows, lengths, sample_prompt, norm_gain, query_weight, *others
        )

    return jax.shard_map(
        local,
        mesh=mesh,
        in_specs=(
            P(None, "ctx", None),
            P(None, "ctx", None),
            P(),
            P("ctx"),
            P(),
            P("ctx", "tp"),
            P(None, "tp"),
            P(None, "tp"),
            P("tp"),
            P("tp"),
            P("tp"),
            P("tp", "ctx"),
            P(None, "ctx", "tp"),
            P(None, "ctx", "tp"),
        ),
        out_specs=(P(None, "ctx", "tp"), P(None, "ctx", "tp")),
        check_vma=False,
    )
```

```python
import functools
import math

import jax
import jax.numpy as jnp
from jax import lax
from jax.experimental import pallas as pl
from jax.experimental.pallas import tpu as pltpu
from jax.sharding import PartitionSpec as P


HEADS = 28
KV_HEADS = 4
HEAD = 128


ROPE_BASE = 1000000.0
NORM_EPS = 1e-06
MASKED = -1e30


def norm_rows(inputs, norm_gain):
    widened = inputs.astype(jnp.float32)
    inverse = lax.rsqrt(jnp.mean(widened * widened, axis=-1, keepdims=True) + NORM_EPS)
    return (widened * inverse * norm_gain).astype(jnp.bfloat16)


def rotate(vectors, positions):
    width = vectors.shape[-1]
    half = width // 2
    exponent = jnp.arange(half, dtype=jnp.float32) * (2.0 / width)
    frequency = jnp.exp(exponent * -math.log(ROPE_BASE))
    angles = positions.astype(jnp.float32)[..., None, None] * frequency
    cosine = jnp.cos(angles)
    sine = jnp.sin(angles)
    first = vectors[..., :half]
    second = vectors[..., half:]
    return jnp.concatenate(
        [first * cosine - second * sine, second * cosine + first * sine], axis=-1
    )


def project(normed, weight, bias):
    return jnp.dot(normed, weight, preferred_element_type=jnp.float32) + bias


def key_positions(count, prefix_dev, span_dev, prefix_all):
    row_index = jnp.arange(count, dtype=jnp.int32)
    device = row_index // (prefix_dev + span_dev)
    offset = row_index % (prefix_dev + span_dev)
    return jnp.where(
        offset < prefix_dev,
        device * prefix_dev + offset,
        prefix_all + device * span_dev + offset - prefix_dev,
    )


def local_gathering(
    span_rows,
    step_rows,
    lengths,
    sample_prompt,
    norm_gain,
    query_weight,
    key_weight,
    value_weight,
    query_bias,
    key_bias,
    value_bias,
    out_weight,
    cache_keys,
    cache_values,
):
    cycle_size = lax.axis_size("ctx")
    cycle_place = lax.axis_index("ctx")
    prompt_count = span_rows.shape[0]
    span_dev = span_rows.shape[1]
    prefix_dev = cache_keys.shape[1]
    kv_local = key_weight.shape[1] // HEAD
    kv_group = HEADS // KV_HEADS
    heads_local = kv_local * kv_group
    prefix_all = prefix_dev * cycle_size
    factor = HEAD ** (-0.5)
    full_query = lax.all_gather(query_weight, "ctx", axis=0, tiled=True)
    normed = norm_rows(span_rows, norm_gain)
    span_places = prefix_all + cycle_place * span_dev + jnp.arange(span_dev, dtype=jnp.int32)
    grid_places = jnp.broadcast_to(span_places, (prompt_count, span_dev))
    queries = rotate(
        project(normed, full_query, query_bias).reshape(prompt_count, span_dev, heads_local, HEAD),
        grid_places,
    ).astype(jnp.bfloat16)
    new_keys = rotate(
        project(normed, key_weight, key_bias).reshape(prompt_count, span_dev, kv_local, HEAD),
        grid_places,
    ).astype(jnp.bfloat16)
    new_values = project(normed, value_weight, value_bias).astype(jnp.bfloat16)
    key_block = jnp.concatenate(
        [cache_keys, new_keys.reshape(prompt_count, span_dev, kv_local * HEAD)], axis=1
    )
    value_block = jnp.concatenate([cache_values, new_values], axis=1)
    query_rows = (
        queries.reshape(prompt_count, span_dev, kv_local, kv_group, HEAD)
        .transpose(0, 2, 1, 3, 4)
        .reshape(prompt_count, kv_local, span_dev * kv_group, HEAD)
    )
    query_places = jnp.repeat(span_places, kv_group)
    row_count = span_dev * kv_group
    highest = jnp.full((prompt_count, kv_local, row_count), MASKED, jnp.float32)
    key_piece = lax.all_gather(key_block, "ctx", axis=1, tiled=True)
    value_piece = lax.all_gather(value_block, "ctx", axis=1, tiled=True)
    count = key_piece.shape[1]
    places = key_positions(count, prefix_dev, span_dev, prefix_all)
    key_grid = key_piece.reshape(prompt_count, count, kv_local, HEAD)
    value_grid = value_piece.reshape(prompt_count, count, kv_local, HEAD)
    scores = (
        jnp.einsum("pgqd,pkgd->pgqk", query_rows, key_grid, preferred_element_type=jnp.float32)
        * factor
    )
    visible = (places[None, None, None, :] < lengths[:, None, None, None]) & (
        places[None, None, None, :] <= query_places[None, None, :, None]
    )
    scores = jnp.where(visible, scores, MASKED)
    raised = jnp.maximum(highest, jnp.max(scores, axis=-1))
    weights = jnp.where(visible, jnp.exp(scores - raised[..., None]), 0.0)
    totals = jnp.sum(weights, axis=-1)
    blended = jnp.einsum(
        "pgqk,pkgd->pgqd",
        weights.astype(jnp.bfloat16),
        value_grid,
        preferred_element_type=jnp.float32,
    )
    highest, totals, blended = (raised, totals, blended)
    key_all, value_all = (
        lax.all_gather(key_block, "ctx", axis=1, tiled=True),
        lax.all_gather(value_block, "ctx", axis=1, tiled=True),
    )
    span_attention = (blended / totals[..., None]).astype(jnp.bfloat16)
    span_attention = (
        span_attention.reshape(prompt_count, kv_local, span_dev, kv_group, HEAD)
        .transpose(0, 2, 1, 3, 4)
        .reshape(prompt_count, span_dev, heads_local * HEAD)
    )
    full_out = lax.all_gather(out_weight, "ctx", axis=1, tiled=True)
    span_terms = jnp.dot(span_attention, full_out, preferred_element_type=jnp.float32)
    span_out = lax.psum_scatter(
        span_terms.astype(jnp.bfloat16), "tp", scatter_dimension=2, tiled=True
    )
    gathered_rows = key_all.shape[1]
    key_grid = key_all.reshape(prompt_count, gathered_rows, kv_local, HEAD)
    value_grid = value_all.reshape(prompt_count, gathered_rows, kv_local, HEAD)
    all_places = key_positions(gathered_rows, prefix_dev, span_dev, prefix_all)
    picked = sample_prompt[:, None] == jnp.arange(prompt_count, dtype=jnp.int32)[None, :]
    length_of = jnp.sum(jnp.where(picked, lengths[None, :], 0), axis=1)
    prefix_visible = picked[:, :, None] & (all_places[None, None, :] < length_of[:, None, None])
    wide_visible = prefix_visible[:, None, None, :, :]
    sample_count = step_rows.shape[1]
    step_count = step_rows.shape[0]
    step_ids = jnp.arange(step_count, dtype=jnp.int32)
    made_keys = jnp.zeros((sample_count, step_count, kv_local, HEAD), jnp.bfloat16)
    made_values = jnp.zeros((sample_count, step_count, kv_local, HEAD), jnp.bfloat16)
    outputs = []
    for step_index in range(step_count):
        normed_step = norm_rows(step_rows[step_index], norm_gain)
        places_now = length_of + step_index
        step_queries = rotate(
            project(normed_step, full_query, query_bias).reshape(sample_count, heads_local, HEAD),
            places_now,
        ).astype(jnp.bfloat16)
        step_queries = step_queries.reshape(sample_count, kv_local, kv_group, HEAD)
        fresh_keys = rotate(
            project(normed_step, key_weight, key_bias).reshape(sample_count, kv_local, HEAD),
            places_now,
        ).astype(jnp.bfloat16)
        fresh_values = (
            project(normed_step, value_weight, value_bias)
            .astype(jnp.bfloat16)
            .reshape(sample_count, kv_local, HEAD)
        )
        made_keys = made_keys.at[:, step_index].set(fresh_keys)
        made_values = made_values.at[:, step_index].set(fresh_values)
        own_visible = step_ids <= step_index
        far_scores = (
            jnp.einsum(
                "sgqd,pkgd->sgqpk", step_queries, key_grid, preferred_element_type=jnp.float32
            )
            * factor
        )
        far_scores = jnp.where(wide_visible, far_scores, MASKED)
        near_scores = (
            jnp.einsum(
                "sgqd,stgd->sgqt", step_queries, made_keys, preferred_element_type=jnp.float32
            )
            * factor
        )
        near_scores = jnp.where(own_visible, near_scores, MASKED)
        highest_now = jnp.maximum(jnp.max(far_scores, axis=(3, 4)), jnp.max(near_scores, axis=-1))
        far_weights = jnp.where(
            wide_visible, jnp.exp(far_scores - highest_now[..., None, None]), 0.0
        )
        near_weights = jnp.where(own_visible, jnp.exp(near_scores - highest_now[..., None]), 0.0)
        totals_now = jnp.sum(far_weights, axis=(3, 4)) + jnp.sum(near_weights, axis=-1)
        blended_now = jnp.einsum(
            "sgqpk,pkgd->sgqd",
            far_weights.astype(jnp.bfloat16),
            value_grid,
            preferred_element_type=jnp.float32,
        )
        blended_now = blended_now + jnp.einsum(
            "sgqt,stgd->sgqd",
            near_weights.astype(jnp.bfloat16),
            made_values,
            preferred_element_type=jnp.float32,
        )
        step_attention = (
            (blended_now / totals_now[..., None])
            .astype(jnp.bfloat16)
            .reshape(sample_count, heads_local * HEAD)
        )
        outputs.append(step_attention)
    stacked = jnp.stack(outputs)
    decode_terms = jnp.dot(stacked, full_out, preferred_element_type=jnp.float32)
    dec_out = lax.psum_scatter(
        decode_terms.astype(jnp.bfloat16), "tp", scatter_dimension=2, tiled=True
    )
    return (span_out, dec_out)


LOG2_E = 1.4426950408889634
VMEM = pl.BlockSpec(memory_space=pltpu.VMEM)
HBM = pl.BlockSpec(memory_space=pltpu.HBM)
SMEM = pl.BlockSpec(memory_space=pltpu.SMEM)
KERNEL = pltpu.CompilerParams(vmem_limit_bytes=16 * 2**20)
NORM_KERNEL = pltpu.CompilerParams(vmem_limit_bytes=66400000)
KEY_VALUE_KERNEL = pltpu.CompilerParams(vmem_limit_bytes=60 * 2**20)


def rotation_tables(positions):
    half = HEAD // 2
    lane = lax.broadcasted_iota(jnp.int32, (1, HEAD), 1)
    exponent = lax.rem(lane, half).astype(jnp.float32) * (2.0 / HEAD)
    frequency = jnp.exp(exponent * -math.log(ROPE_BASE))
    angles = positions.astype(jnp.float32) * frequency
    sine = jnp.sin(angles)
    return jnp.cos(angles), jnp.where(lane < half, -sine, sine)


def rotate_block(block, cosine, sine):
    return block * cosine + pltpu.roll(block, HEAD // 2, 1) * sine


def fetch_all(sources, targets, semaphores):
    copies = [
        pltpu.make_async_copy(source, target, semaphores.at[index])
        for index, (source, target) in enumerate(zip(sources, targets))
    ]
    for copy in copies:
        copy.start()
    for copy in copies:
        copy.wait()


def norm_kernel(place_ref, span_hbm, step_hbm, gain_hbm, *rest):
    *message_refs, normed_ref, widened, span_ref, step_ref, gain_ref, semaphores = rest
    fetch_all((span_hbm, step_hbm, gain_hbm), (span_ref, step_ref, gain_ref), semaphores)
    prompts, span_dev, _ = span_ref.shape
    steps, samples, _ = step_ref.shape
    for prompt in range(prompts):
        widened[prompt * span_dev : (prompt + 1) * span_dev, :] = span_ref[prompt].astype(
            jnp.float32
        )
    base = prompts * span_dev
    for step in range(steps):
        widened[base + step * samples : base + (step + 1) * samples, :] = step_ref[step].astype(
            jnp.float32
        )
    rows = widened[...]
    inverse = lax.rsqrt(jnp.mean(rows * rows, axis=-1, keepdims=True) + NORM_EPS)
    normed_ref[...] = (rows * inverse * gain_ref[...][None, :]).astype(jnp.bfloat16)
    width = message_refs[0].shape[1]
    for slot, message_ref in enumerate(message_refs):
        start = pl.multiple_of((place_ref[0] ^ slot) * width, width)
        message_ref[...] = normed_ref[:, pl.ds(start, width)]


def key_value_kernel(
    steps,
    ctx_ref,
    lengths_ref,
    sample_prompt_ref,
    *rest,
):
    chips = (len(rest) - 16) // 2
    message_hbm, rest = rest[:chips], rest[chips:]
    (key_weight_hbm, value_weight_hbm, *other_hbm), rest = rest[:6], rest[6:]
    (packed_ref, own_ref, cosine_ref, sine_ref), rest = rest[:4], rest[4:]
    message_refs, (weight_ref, *fetched, semaphores) = rest[:chips], rest[chips:]
    key_bias_ref, value_bias_ref, cache_keys_ref, cache_values_ref = fetched[:4]
    prompts, prefix_dev, width = cache_keys_ref.shape
    copies = [
        pltpu.make_async_copy(source, target, semaphores.at[index])
        for index, (source, target) in enumerate(
            [
                (key_weight_hbm, weight_ref.at[:, :width]),
                (value_weight_hbm, weight_ref.at[:, width:]),
            ]
            + list(zip(other_hbm, fetched))
            + list(zip(message_hbm, message_refs))
        )
    ]
    for copy in copies:
        copy.start()
    samples = sample_prompt_ref.shape[0]
    own_rows = steps * samples
    row_count, chip_width = message_refs[0].shape
    span_dev = (row_count - own_rows) // prompts
    block = prefix_dev + span_dev
    row_index = lax.broadcasted_iota(jnp.int32, (row_count, 1), 0)
    span_start = (2 * chips * prefix_dev) + ctx_ref[0] * span_dev
    positions = span_start + lax.rem(row_index, span_dev)
    own_index = row_index - prompts * span_dev
    for index in range(samples):
        start = lengths_ref[sample_prompt_ref[index]]
        taken = (own_index >= 0) & (lax.rem(own_index, samples) == index)
        positions = jnp.where(taken, start + lax.div(own_index, samples), positions)
    cosine, sine = rotation_tables(positions)
    cosine_ref[...], sine_ref[...] = cosine, sine
    for copy in copies:
        copy.wait()
    products = None
    for slot, message_ref in enumerate(message_refs):
        start = pl.multiple_of((lax.div(ctx_ref[0], 2) ^ slot) * chip_width, chip_width)
        product = jnp.dot(
            message_ref[...],
            weight_ref[pl.ds(start, chip_width), :],
            preferred_element_type=jnp.float32,
        )
        products = product if products is None else products + product
    keys = products[:, :width] + key_bias_ref[...][None, :]
    values = (products[:, width:] + value_bias_ref[...][None, :]).astype(jnp.bfloat16)
    keys = jnp.concatenate(
        [
            rotate_block(keys[:, at : at + HEAD], cosine, sine)
            for at in range(0, width, HEAD)
        ],
        axis=1,
    ).astype(jnp.bfloat16)
    for kind, (cache_ref, fresh) in enumerate(
        ((cache_keys_ref, keys), (cache_values_ref, values))
    ):
        for prompt in range(prompts):
            start = (kind * prompts + prompt) * block
            packed_ref[start : start + prefix_dev, :] = cache_ref[prompt]
            packed_ref[start + prefix_dev : start + block, :] = fresh[
                prompt * span_dev : (prompt + 1) * span_dev
            ]
        own_ref[kind] = fresh[prompts * span_dev :]


def query_kernel(core_ref, rows_ref, own_ref, other_ref, out_ref):
    half = own_ref.shape[0]

    def product(first_ref, second_ref):
        total = jnp.dot(rows_ref[:, :half], first_ref[...], preferred_element_type=jnp.float32)
        total = total + jnp.dot(
            rows_ref[:, half:], second_ref[...], preferred_element_type=jnp.float32
        )
        out_ref[...] = total.astype(out_ref.dtype)

    @pl.when(core_ref[0] == 0)
    def _():
        product(own_ref, other_ref)

    @pl.when(core_ref[0] == 1)
    def _():
        product(other_ref, own_ref)


def turn_kernel(core_ref, own_ref, other_ref, out_ref):
    half = own_ref.shape[0]

    @pl.when(core_ref[0] == 0)
    def _():
        out_ref[:, :half] = own_ref[...].T
        out_ref[:, half:] = other_ref[...].T

    @pl.when(core_ref[0] == 1)
    def _():
        out_ref[:, :half] = other_ref[...].T
        out_ref[:, half:] = own_ref[...].T


def out_kernel(rows_ref, weight_ref, out_ref):
    out_ref[...] = jnp.dot(
        rows_ref[...], weight_ref[...], preferred_element_type=jnp.float32
    ).astype(out_ref.dtype)


def own_query_kernel(
    prefix_dev,
    group,
    core_ref,
    ctx_ref,
    lengths_ref,
    sample_prompt_ref,
    rows_ref,
    own_ref,
    other_ref,
    bias_ref,
    *rest,
):
    staged_refs, share_ref, rest = rest[:3], rest[3], rest[4:]
    staged_outs, span_limit_ref, step_limit_ref = rest[:3], rest[3], rest[4]
    query_kernel(core_ref, rows_ref, own_ref, other_ref, share_ref)
    share_ref[...] += bias_ref[...][None, :]
    for staged_ref, staged_out in zip(staged_refs, staged_outs):
        staged_out[...] = staged_ref[...]
    prompts, span_rows, _ = span_limit_ref.shape
    own_rows = staged_refs[2].shape[1]
    samples = sample_prompt_ref.shape[0]
    span_dev = span_rows // group
    row_index = lax.broadcasted_iota(jnp.int32, (span_rows, 1), 0)
    query_places = ctx_ref[1] * prefix_dev + ctx_ref[0] * span_dev + lax.rem(row_index, span_dev)
    row_index = lax.broadcasted_iota(jnp.int32, (group * own_rows, 1), 0)
    sample = lax.rem(row_index, samples)
    for prompt in range(prompts):
        span_limit_ref[prompt] = jnp.minimum(query_places, lengths_ref[prompt] - 1)
        limit = jnp.full(row_index.shape, -1, jnp.int32)
        for index in range(samples):
            reach = jnp.where(sample_prompt_ref[index] == prompt, lengths_ref[prompt] - 1, -1)
            limit = jnp.where(sample == index, reach, limit)
        step_limit_ref[prompt] = limit


def attend_kernel(
    steps,
    prefix_dev,
    ctx_ref,
    span_limit_ref,
    step_limit_ref,
    cosine_ref,
    sine_ref,
    own_ref,
    *rest,
):
    *query_refs, near_ref, far_ref, out_ref, rotated = rest
    packed_refs = (near_ref, far_ref)
    prompts = span_limit_ref.shape[0]
    own_rows, kv_width = own_ref.shape[1:]
    samples = own_rows // steps
    row_count, columns = out_ref.shape
    span_dev = (row_count - own_rows) // prompts
    kv_local = kv_width // HEAD
    heads_local = columns // HEAD
    group = heads_local // kv_local
    scale = HEAD ** (-0.5) * LOG2_E
    cosine, sine = cosine_ref[...], sine_ref[...]
    for head in range(heads_local):
        span = slice(head * HEAD, (head + 1) * HEAD)
        total = query_refs[0][:, span].astype(jnp.float32)
        for query_ref in query_refs[1:]:
            total = total + query_ref[:, span].astype(jnp.float32)
        rotated[:, span] = rotate_block(total, cosine, sine).astype(jnp.bfloat16)
    chips, packed_rows, _ = near_ref.shape
    block = packed_rows // (2 * prompts)
    prefix_all = 2 * chips * prefix_dev
    key_index = lax.broadcasted_iota(jnp.int32, (1, 2 * chips * block), 1)
    slot, offset = lax.div(key_index, block), lax.rem(key_index, block)
    owner = ctx_ref[0] ^ (2 * lax.rem(slot, chips) + lax.div(slot, chips))
    places = jnp.where(
        offset < prefix_dev,
        owner * prefix_dev + offset,
        prefix_all + owner * span_dev + offset - prefix_dev,
    )

    def rows_of(start, count, first_head):
        return jnp.concatenate(
            [
                rotated[start : start + count, head * HEAD : (head + 1) * HEAD]
                for head in range(first_head, first_head + group)
            ],
            axis=0,
        )

    def cached(kind, prompt, group_index):
        start = (kind * prompts + prompt) * block
        lanes = slice(group_index * HEAD, (group_index + 1) * HEAD)
        return jnp.concatenate(
            [
                packed_ref[index, start : start + block, lanes]
                for packed_ref in packed_refs
                for index in range(packed_ref.shape[0])
            ],
            axis=0,
        )

    def score(queries, keys, visible):
        raw = lax.dot_general(
            queries, keys, (((1,), (1,)), ((), ())), preferred_element_type=jnp.float32
        )
        return jnp.where(visible, raw * scale, MASKED)

    def store(start, count, first_head, blended):
        for offset in range(group):
            head = first_head + offset
            out_ref[start : start + count, head * HEAD : (head + 1) * HEAD] = blended[
                offset * count : (offset + 1) * count
            ]

    for group_index in range(kv_local):
        first_head = group_index * group
        keys = [cached(0, prompt, group_index) for prompt in range(prompts)]
        values = [cached(1, prompt, group_index) for prompt in range(prompts)]
        for prompt in range(prompts):
            queries = rows_of(prompt * span_dev, span_dev, first_head)
            scores = score(queries, keys[prompt], places <= span_limit_ref[prompt])
            highest = jnp.max(scores, axis=-1, keepdims=True)
            weights = jnp.exp2(scores - highest)
            totals = jnp.sum(weights, axis=-1, keepdims=True)
            blended = jnp.dot(
                weights.astype(jnp.bfloat16), values[prompt], preferred_element_type=jnp.float32
            )
            store(
                prompt * span_dev, span_dev, first_head, (blended / totals).astype(jnp.bfloat16)
            )
        start = prompts * span_dev
        queries = rows_of(start, own_rows, first_head)
        row_index = lax.rem(lax.broadcasted_iota(jnp.int32, (group * own_rows, 1), 0), own_rows)
        sample = lax.rem(row_index, samples)
        step = lax.div(row_index, samples)
        own_index = lax.broadcasted_iota(jnp.int32, (1, own_rows), 1)
        own_visible = (lax.rem(own_index, samples) == sample) & (
            lax.div(own_index, samples) <= step
        )
        own_lanes = slice(group_index * HEAD, (group_index + 1) * HEAD)
        parts = [score(queries, own_ref[0, :, own_lanes], own_visible)]
        for prompt in range(prompts):
            parts.append(score(queries, keys[prompt], places <= step_limit_ref[prompt]))
        highest = functools.reduce(
            jnp.maximum, [jnp.max(part, axis=-1, keepdims=True) for part in parts]
        )
        weights = [jnp.exp2(part - highest) for part in parts]
        totals = sum(jnp.sum(weight, axis=-1, keepdims=True) for weight in weights)
        blended = sum(
            jnp.dot(weight.astype(jnp.bfloat16), value, preferred_element_type=jnp.float32)
            for weight, value in zip(weights, [own_ref[1, :, own_lanes]] + values)
        )
        store(start, own_rows, first_head, (blended / totals).astype(jnp.bfloat16))


def add_kernel(*refs):
    share_refs, span_ref, step_ref = refs[:-2], refs[-2], refs[-1]
    prompts, span_dev, _ = span_ref.shape
    steps, samples, _ = step_ref.shape
    total = share_refs[0][...].astype(jnp.float32)
    for share_ref in share_refs[1:]:
        total = total + share_ref[...].astype(jnp.float32)
    for prompt in range(prompts):
        rows = slice(prompt * span_dev, (prompt + 1) * span_dev)
        span_ref[prompt] = total[rows].astype(jnp.bfloat16)
    for step in range(steps):
        start = prompts * span_dev + step * samples
        step_ref[step] = total[start : start + samples].astype(jnp.bfloat16)


def local_moving_rows(
    span_rows,
    step_rows,
    lengths,
    sample_prompt,
    norm_gain,
    query_weight,
    key_weight,
    value_weight,
    query_bias,
    key_bias,
    value_bias,
    out_weight,
    cache_keys,
    cache_values,
):
    ctx_size = lax.axis_size("ctx")
    tp_size = lax.axis_size("tp")
    ctx_place = lax.axis_index("ctx")
    tp_place = lax.axis_index("tp")
    chip_place, core_place = ctx_place // 2, ctx_place % 2
    chips = ctx_size // 2
    prompts, span_dev, model = span_rows.shape
    steps, samples, _ = step_rows.shape
    prefix_dev, kv_width = cache_keys.shape[1:]
    columns = query_weight.shape[1]
    row_count = prompts * span_dev + steps * samples
    chip_width = model // chips
    core_pairs = [(place, place ^ 1) for place in range(ctx_size)]

    def to_chip(block, slot):
        return lax.ppermute(
            block, "ctx", [(place, place ^ (2 * slot)) for place in range(ctx_size)]
        )

    bf16 = functools.partial(jax.ShapeDtypeStruct, dtype=jnp.bfloat16)
    messages = pl.pallas_call(
        norm_kernel,
        out_shape=[bf16((row_count, chip_width))] * chips,
        in_specs=[SMEM, HBM, HBM, HBM],
        out_specs=[VMEM] * chips,
        scratch_shapes=[
            pltpu.VMEM((row_count, model), jnp.bfloat16),
            pltpu.VMEM((row_count, model), jnp.float32),
            pltpu.VMEM(span_rows.shape, jnp.bfloat16),
            pltpu.VMEM(step_rows.shape, jnp.bfloat16),
            pltpu.VMEM(norm_gain.shape, jnp.float32),
            pltpu.SemaphoreType.DMA((3,)),
        ],
        compiler_params=NORM_KERNEL,
        name="norm",
    )(chip_place.reshape(1), span_rows, step_rows, norm_gain)
    inbound = [messages[0]] + [to_chip(messages[slot], slot) for slot in range(1, chips)]
    other_query = lax.ppermute(query_weight, "ctx", core_pairs)
    other_out = lax.ppermute(out_weight.T, "ctx", core_pairs)
    block = prefix_dev + span_dev
    table = jax.ShapeDtypeStruct((row_count, HEAD), jnp.float32)
    packed, own, cosine, sine = pl.pallas_call(
        functools.partial(key_value_kernel, steps),
        out_shape=[
            bf16((2 * prompts * block, kv_width)),
            bf16((2, steps * samples, kv_width)),
            table,
            table,
        ],
        in_specs=[SMEM] * 3 + [HBM] * (chips + 6),
        out_specs=[VMEM] * 4,
        scratch_shapes=[pltpu.VMEM((row_count, chip_width), jnp.bfloat16)] * chips
        + [pltpu.VMEM((model, 2 * kv_width), jnp.bfloat16)]
        + [
            pltpu.VMEM(array.shape, array.dtype)
            for array in (key_bias, value_bias, cache_keys, cache_values)
        ]
        + [pltpu.SemaphoreType.DMA((chips + 6,))],
        compiler_params=KEY_VALUE_KERNEL,
        name="key_value",
    )(
        ctx_place.reshape(1),
        lengths,
        sample_prompt,
        *messages,
        key_weight,
        value_weight,
        key_bias,
        value_bias,
        cache_keys,
        cache_values,
    )
    near_packed = jnp.stack([packed] + [to_chip(packed, slot) for slot in range(1, chips)])
    far_packed = lax.ppermute(near_packed, "ctx", core_pairs)

    shares, later = [], []
    group = columns // kv_width
    for slot, rows in enumerate(inbound):
        weights = (core_place.reshape(1), rows, query_weight, other_query)
        if slot:
            partial = pl.pallas_call(
                query_kernel,
                out_shape=bf16((row_count, columns)),
                in_specs=[SMEM] + [VMEM] * 3,
                out_specs=VMEM,
                compiler_params=KERNEL,
                name="query_dot",
            )(*weights)
        else:
            partial, *later = pl.pallas_call(
                functools.partial(own_query_kernel, prefix_dev, group),
                out_shape=[
                    jax.ShapeDtypeStruct((row_count, columns), jnp.float32),
                    table,
                    table,
                    bf16(own.shape),
                    jax.ShapeDtypeStruct((prompts, group * span_dev, 1), jnp.int32),
                    jax.ShapeDtypeStruct((prompts, group * steps * samples, 1), jnp.int32),
                ],
                in_specs=[SMEM] * 4 + [VMEM] * 7,
                out_specs=[VMEM] * 6,
                compiler_params=KERNEL,
                name="query_own",
            )(
                core_place.reshape(1),
                jnp.stack([ctx_place, jnp.int32(ctx_size)]),
                lengths,
                sample_prompt,
                *weights[1:],
                query_bias,
                cosine,
                sine,
                own,
            )
        if slot:
            partial = to_chip(partial, slot)
        shares.append(partial)
    cosine, sine, own, span_limit, step_limit = later

    attention = pl.pallas_call(
        functools.partial(attend_kernel, steps, prefix_dev),
        out_shape=bf16((row_count, columns)),
        in_specs=[SMEM] + [VMEM] * (5 + chips + 2),
        out_specs=VMEM,
        scratch_shapes=[pltpu.VMEM((row_count, columns), jnp.bfloat16)],
        compiler_params=KERNEL,
        name="attend",
    )(
        ctx_place.reshape(1),
        span_limit,
        step_limit,
        cosine,
        sine,
        own,
        *shares,
        near_packed,
        far_packed,
    )

    chip_out = pl.pallas_call(
        turn_kernel,
        out_shape=bf16((columns, 2 * out_weight.shape[1])),
        in_specs=[SMEM] + [VMEM] * 2,
        out_specs=VMEM,
        compiler_params=KERNEL,
        name="out_turn",
    )(core_place.reshape(1), out_weight.T, other_out)
    attended = [attention] + [to_chip(attention, slot) for slot in range(1, chips)]
    returned = []
    for slot, rows in enumerate(attended):
        terms = pl.pallas_call(
            out_kernel,
            out_shape=bf16((row_count, columns)),
            in_specs=[VMEM] * 2,
            out_specs=VMEM,
            compiler_params=KERNEL,
            name="out_dot",
        )(rows, chip_out)
        if slot:
            terms = to_chip(terms, slot)
        returned.append(terms)
    returned = jnp.stack(returned)

    def columns_of(slot):
        return lax.dynamic_index_in_dim(returned, tp_place ^ slot ^ chip_place, 0, keepdims=False)

    finals = [columns_of(0)]
    for slot in range(1, tp_size):
        finals.append(
            lax.ppermute(
                columns_of(slot), "tp", [(place, place ^ slot) for place in range(tp_size)]
            )
        )
    return pl.pallas_call(
        add_kernel,
        out_shape=[bf16((prompts, span_dev, columns)), bf16((steps, samples, columns))],
        in_specs=[VMEM] * tp_size,
        out_specs=[VMEM] * 2,
        compiler_params=KERNEL,
        name="add",
    )(*finals)


def rows_are_lighter(mesh, rows, model):
    ctx_size, tp_size = mesh.shape["ctx"], mesh.shape["tp"]
    fits = ctx_size == 2 * tp_size and tp_size & (tp_size - 1) == 0
    return fits and rows < model


def solution(mesh):
    def local(span_rows, step_rows, lengths, sample_prompt, norm_gain, query_weight, *others):
        whole_rows = (span_rows.shape[0] * span_rows.shape[1], step_rows.shape[0] * step_rows.shape[1])
        rows = sum(whole_rows) * mesh.shape["ctx"]
        form = local_gathering
        if rows_are_lighter(mesh, rows, query_weight.shape[0] * mesh.shape["ctx"]):
            form = local_moving_rows
        return form(
            span_rows, step_rows, lengths, sample_prompt, norm_gain, query_weight, *others
        )

    return jax.shard_map(
        local,
        mesh=mesh,
        in_specs=(
            P(None, "ctx", None),
            P(None, "ctx", None),
            P(),
            P("ctx"),
            P(),
            P("ctx", "tp"),
            P(None, "tp"),
            P(None, "tp"),
            P("tp"),
            P("tp"),
            P("tp"),
            P("tp", "ctx"),
            P(None, "ctx", "tp"),
            P(None, "ctx", "tp"),
        ),
        out_specs=(P(None, "ctx", "tp"), P(None, "ctx", "tp")),
        check_vma=False,
    )
```
